256 devices in a mesh: gz: 16 (over z, y_lo), gy: 16 (over x, y_hi, core).
Axes of the slice: x: 4, y: 4 (y_hi: 2, y_lo: 2; y = y_hi * 2 + y_lo), z: 8, core: 2. Of those that a mesh axis runs over, the one named last changes fastest.
Arguments:
- charge: float32 [3145728], P(('gz', 'gy')), may hold values from -4 to 4
- fractions: float32 [3, 3145728], P(None, ('gz', 'gy')), may hold values from 0 to 1
- cell_base: int32 [3, 3145728], P(None, ('gz', 'gy')), may hold values from 0 to 255, as said below
- live_blocks: int32 [16, 16], P('gz'), may hold values from 12 to 96, as said below
- send_blocks: int32 [16, 16], P('gz'), may hold values from 0 to 36, as said below
- moduli: float32 [3, 256], replicated, may hold values from 0.5 to 2
- screening: float32 [1], replicated, may hold values from 8 to 16
Outputs:
- forces: float32 [3, 3145728], P(None, ('gz', 'gy'))
The draws below stay inside these ranges and needn't reach their ends.
Inputs may be any that keep to these rules, and one draw needn't show every extreme that they name: `cell_base`: row 0 lies in 0 to 15, row 1 in 0 to 15, row 2 in 0 to 255. `live_blocks`: a domain's live blocks are its first ones; in every row of the table some domain has 96 live blocks. send_blocks is at most the domain's live blocks; live_blocks minus send_blocks plus send_blocks of the domain before it along gy (cyclically) is at most 96; in every row some domain sends 36.
All inputs are finite; a program needn't handle non-finite values.
Results may differ from the reference program's by a relative error of at most 0.00023.
Values sent between devices are 32-bit elements; how exact they have to be, the bound alone decides.
A program may use at most 64 MiB of HBM per device.

```python
import math
import jax
import jax.numpy as jnp

GRID = 256
BLOCK = 128
NBLK = 96
ATOMS_DEV = 12288
ATOMS = 3145728
PZ = 16
PY = 16
SEND_MAX = 36
LOW = 12
N_GZ = 16
N_GY = 16


def migration_plan(key):
    base_key = jax.random.fold_in(key, 7)
    key_load, key_busy = jax.random.split(base_key)
    drawn = jax.random.randint(key_load, (N_GZ, N_GY), 0, 1001)
    powered = drawn * drawn // 1000
    powered = powered * powered // 1000
    live_count = LOW + (NBLK - LOW) * powered // 1000
    busiest = jax.random.randint(key_busy, (N_GZ, 1), 0, N_GY)
    lane_ids = jnp.arange(N_GY, dtype=jnp.int32)[None, :]
    live_count = jnp.where(lane_ids == busiest, NBLK, live_count)
    live_count = jnp.where(lane_ids == jnp.mod(busiest + 1, N_GY), LOW, live_count)
    following = jnp.roll(live_count, -1, axis=1)
    send_count = jnp.clip((live_count - following + 1) // 2, 0, SEND_MAX)
    return (live_count.astype(jnp.int32), send_count.astype(jnp.int32))


def draw_live_blocks(key, part):
    return migration_plan(key)[0]


def draw_send_blocks(key, part):
    return migration_plan(key)[1]


def draw_cell_base(key, part):
    key_z, key_y, key_x = jax.random.split(jax.random.fold_in(key, 11), 3)
    rows_z = jax.random.randint(key_z, (ATOMS,), 0, PZ)
    rows_y = jax.random.randint(key_y, (ATOMS,), 0, PY)
    rows_x = jax.random.randint(key_x, (ATOMS,), 0, GRID)
    return jnp.stack([rows_z, rows_y, rows_x]).astype(jnp.int32)


def steps_of(key, extent, cuts, low, high):
    def one(axis_at, shards_of):
        draws = jax.random.uniform(jax.random.fold_in(jax.random.fold_in(key, 6), axis_at), (shards_of,), jnp.float32, low / len(cuts), high / len(cuts))
        return jnp.repeat(jnp.exp(draws), extent[axis_at] // shards_of).reshape((-1,) + (1,) * (len(extent) - axis_at - 1))

    level = one(*cuts[0])
    for cut in cuts[1:]:
        level = level * one(*cut)
    return level


def normal_values(stream_key, shape, scale, limit, shards=(), held_as=jnp.bfloat16):
    factor_of = steps_of(stream_key, shape, shards, -0.22, 0.18) if shards else 1.0
    array = jax.random.normal(stream_key, shape, jnp.float32) * scale * factor_of
    return jnp.minimum(jnp.maximum(array, -limit), limit).astype(held_as)


def setup_inputs(seed: int = 0) -> dict:
    splits = jax.random.split(jax.random.key(seed), 8)
    charge = normal_values(splits[0], (ATOMS,), 1.0, 4.0, ((0, 256),), jnp.float32)
    fractions = jnp.clip(1.0 * jax.random.uniform(splits[1], (3, ATOMS), jnp.float32) ** steps_of(splits[1], (3, ATOMS), ((1, 256),), -0.2, 0.2), 0.0, 1.0)
    cell_base = draw_cell_base(jax.random.fold_in(splits[7], 71), 0)
    live_blocks = draw_live_blocks(jax.random.fold_in(splits[7], 71), 0)
    send_blocks = draw_send_blocks(jax.random.fold_in(splits[7], 71), 0)
    moduli = jnp.clip(jnp.exp(jax.random.uniform(splits[5], (3, GRID), jnp.float32, math.log(0.5), math.log(2.0))), 0.5, 2.0)
    screening = jnp.clip(jnp.exp(jax.random.uniform(splits[6], (1,), jnp.float32, math.log(8.0), math.log(16.0))), 8.0, 16.0)
    return {"charge": charge, "fractions": fractions, "cell_base": cell_base, "live_blocks": live_blocks, "send_blocks": send_blocks, "moduli": moduli, "screening": screening}


coulomb = 2.0


def spline_weights(fractions_row):
    remain = 1.0 - fractions_row
    square = fractions_row * fractions_row
    cubed = square * fractions_row
    weights = [remain * remain * remain / 6.0,
               (3.0 * cubed - 6.0 * square + 4.0) / 6.0,
               (-3.0 * cubed + 3.0 * square + 3.0 * fractions_row + 1.0) / 6.0,
               cubed / 6.0]
    slopes = [-0.5 * remain * remain,
              1.5 * square - 2.0 * fractions_row,
              -1.5 * square + fractions_row + 0.5,
              0.5 * square]
    return weights, slopes


def reference(charge, fractions, cell_base, live_blocks, send_blocks, moduli, screening):
    atom_index = jnp.arange(ATOMS, dtype=jnp.int32)
    device_index = atom_index // ATOMS_DEV
    slab_index = device_index // N_GY
    column_index = device_index % N_GY
    slot_index = atom_index % ATOMS_DEV
    live_count = live_blocks[slab_index, column_index]
    weighted = jnp.where(slot_index // BLOCK < live_count, charge, 0.0)
    weight_z, slope_z = spline_weights(fractions[0])
    weight_y, slope_y = spline_weights(fractions[1])
    weight_x, slope_x = spline_weights(fractions[2])
    base_z = slab_index * PZ + cell_base[0]
    base_y = column_index * PY + cell_base[1]
    base_x = cell_base[2]
    density = jnp.zeros((GRID * GRID * GRID,), jnp.float32)
    for shift_z in range(4):
        index_z = jnp.mod(base_z + shift_z, GRID)
        for shift_y in range(4):
            index_y = jnp.mod(base_y + shift_y, GRID)
            for shift_x in range(4):
                index_x = jnp.mod(base_x + shift_x, GRID)
                flat_index = ((index_z * GRID + index_y) * GRID + index_x).astype(jnp.int32)
                density = density.at[flat_index].add(weighted * weight_z[shift_z] * weight_y[shift_y] * weight_x[shift_x])
    density = density.reshape(GRID, GRID, GRID)
    spectrum = jnp.fft.fftn(density)
    waves = jnp.arange(GRID, dtype=jnp.int32)
    signed_wave = jnp.where(waves < GRID // 2, waves, waves - GRID)
    wave_square = signed_wave * signed_wave
    radius = wave_square[:, None, None] + wave_square[None, :, None] + wave_square[None, None, :]
    squared = radius.astype(jnp.float32) / float(GRID * GRID)
    product = coulomb * moduli[0][:, None, None] * moduli[1][None, :, None] * moduli[2][None, None, :]
    safe_squared = jnp.where(radius > 0, squared, 1.0)
    kernel = jnp.where(radius > 0, product * jnp.exp(-screening[0] * squared) / safe_squared, 0.0)
    potential = jnp.real(jnp.fft.ifftn(spectrum * kernel)).astype(jnp.float32)
    flat_potential = potential.reshape(-1)
    force_z = jnp.zeros((ATOMS,), jnp.float32)
    force_y = jnp.zeros((ATOMS,), jnp.float32)
    force_x = jnp.zeros((ATOMS,), jnp.float32)
    for shift_z in range(4):
        index_z = jnp.mod(base_z + shift_z, GRID)
        for shift_y in range(4):
            index_y = jnp.mod(base_y + shift_y, GRID)
            for shift_x in range(4):
                index_x = jnp.mod(base_x + shift_x, GRID)
                flat_index = ((index_z * GRID + index_y) * GRID + index_x).astype(jnp.int32)
                values = flat_potential[flat_index]
                force_z = force_z + slope_z[shift_z] * weight_y[shift_y] * weight_x[shift_x] * values
                force_y = force_y + weight_z[shift_z] * slope_y[shift_y] * weight_x[shift_x] * values
                force_x = force_x + weight_z[shift_z] * weight_y[shift_y] * slope_x[shift_x] * values
    home = -weighted[None, :] * jnp.stack([force_z, force_y, force_x])
    domains = N_GZ * N_GY
    home = home.reshape(3, domains, ATOMS_DEV)
    live_flat = live_blocks.reshape(-1)
    send_flat = send_blocks.reshape(-1)
    devices = jnp.arange(domains, dtype=jnp.int32)
    column_of = devices % N_GY
    previous = (devices - column_of + jnp.mod(column_of - 1, N_GY)).astype(jnp.int32)
    kept_atoms = (live_flat - send_flat) * BLOCK
    arriving = send_flat[previous] * BLOCK
    source_start = (live_flat[previous] - send_flat[previous]) * BLOCK
    slots = jnp.arange(ATOMS_DEV, dtype=jnp.int32)
    own_forces = jnp.where(slots[None, None, :] < kept_atoms[None, :, None], home, 0.0)
    guest_slot = slots[None, :] - kept_atoms[:, None] + source_start[:, None]
    valid = (slots[None, :] >= kept_atoms[:, None]) & (slots[None, :] < kept_atoms[:, None] + arriving[:, None])
    guest_slot = jnp.clip(guest_slot, 0, ATOMS_DEV - 1).astype(jnp.int32)
    neighbour = home[:, previous, :]
    guest = jnp.take_along_axis(neighbour, guest_slot[None, :, :], axis=2)
    result = own_forces + jnp.where(valid[None, :, :], guest, 0.0)
    return result.reshape(3, ATOMS)
```

```python
import functools

import jax
import jax.numpy as jnp
import numpy as np
from jax import lax
from jax.experimental import pallas as pl
from jax.experimental.pallas import tpu as pltpu
from jax.sharding import PartitionSpec as P

GRID = 256
BLOCK = 128
ATOMS_DEV = 12288
SEND_MAX = 36
NPEER = 16
CHUNK = 512
ROWS = 384
MSG_Z = 40
MSG_Y = 32
MESH = pl.DeviceIdType.MESH
BF16 = jnp.bfloat16
F32 = jnp.float32


def split_np(table):
    table = np.asarray(table, np.float32)
    high = table.astype(jnp.bfloat16)
    low = (table - high.astype(np.float32)).astype(jnp.bfloat16)
    return high, low


def kz_of(block, local):
    j = 8 * block + local // 2
    return np.where(local % 2 == 0, j, np.where(j == 0, 128, (256 - j) % 256))


def forward_x():
    x = np.arange(256)[:, None]
    k = np.arange(128)[None, :]
    angle = 2 * np.pi * ((x * k) % 256) / 256
    table = np.concatenate([np.cos(angle), -np.sin(angle)], 1)
    table[:, 128] = (-1.0) ** np.arange(256)
    return table


def inverse_x():
    k = np.arange(128)[:, None]
    x = np.arange(256)[None, :]
    angle = 2 * np.pi * ((x * k) % 256) / 256
    table = np.concatenate([2 * np.cos(angle), -2 * np.sin(angle)], 0) / 256
    table[0] = 1.0 / 256
    table[128] = (-1.0) ** np.arange(256) / 256
    return table


def message_rows_z():
    part = np.zeros(MSG_Z, np.int64)
    place = np.zeros(MSG_Z, np.int64)
    for c in range(2):
        part[16 * c : 16 * c + 16] = c
        place[16 * c : 16 * c + 16] = np.arange(16)
        part[32 + 4 * c : 36 + 4 * c] = c
        place[32 + 4 * c : 36 + 4 * c] = 16 + np.arange(4)
    return part, place


def complex_table(part_out, wave, part_in, place):
    angle = 2 * np.pi * ((wave[:, None] * place[None, :]) % 256) / 256
    cosine, sine = np.cos(angle), np.sin(angle)
    same = part_out[:, None] == part_in[None, :]
    sign = np.where(part_out[:, None] == 0, 1.0, -1.0)
    return np.where(same, cosine, sign * sine)


def forward_z():
    local, part, block = np.meshgrid(np.arange(16), np.arange(2), np.arange(16), indexing="ij")
    wave = kz_of(block, local).reshape(-1)
    part = part.reshape(-1)
    part_in, place = message_rows_z()
    place_all = (16 * np.arange(16)[:, None] + place[None, :]).reshape(-1)
    table = complex_table(part, wave, np.tile(part_in, 16), place_all)
    pad = np.tile(place == 19, 16)
    return np.where(pad[None, :], 0.0, table)


def forward_y():
    part, wave = np.meshgrid(np.arange(2), np.arange(256), indexing="ij")
    block, part_in, place = np.meshgrid(np.arange(16), np.arange(2), np.arange(16), indexing="ij")
    return complex_table(
        part.reshape(-1), wave.reshape(-1), part_in.reshape(-1), (16 * block + place).reshape(-1)
    )


def split(value):
    high = value.astype(BF16)
    low = (value - high.astype(F32)).astype(BF16)
    return high, low


def spline_weights(t):
    remain = 1.0 - t
    square = t * t
    cubed = square * t
    sixth = 1.0 / 6.0
    weights = [
        remain * remain * remain * sixth,
        (3.0 * cubed - 6.0 * square + 4.0) * sixth,
        (-3.0 * cubed + 3.0 * square + 3.0 * t + 1.0) * sixth,
        cubed * sixth,
    ]
    return weights


def spline_slopes(t):
    remain = 1.0 - t
    square = t * t
    return [
        -0.5 * remain * remain,
        1.5 * square - 2.0 * t,
        -1.5 * square + t + 0.5,
        0.5 * square,
    ]


def wide(row, count):
    return jnp.broadcast_to(row, (count, row.shape[1]))


def stencil(rows, offset, cell, weights):
    place = offset - wide(cell, rows)
    table = jnp.zeros((rows, cell.shape[1]), F32)
    for k in range(3, -1, -1):
        table = jnp.where(place == k, wide(weights[k], rows), table)
    return table


def narrow_tables(cells, weights, row):
    n = cells.shape[1]
    cell = cells[row : row + 1]
    picked = [w[row : row + 1] for w in weights]
    iota = lax.broadcasted_iota(jnp.int32, (16, n), 0)
    main = stencil(16, iota, cell, picked)
    halo = stencil(8, 16 + (iota[:8] & 3), cell, picked)
    return main, halo


def x_table(hi_refs_pairs, cells, n):
    cell = cells[2:3]
    keys = [wide(((cell + m) & 255).astype(F32), 16).astype(BF16) for m in range(4)]
    sets = []
    for ref, weights in hi_refs_pairs:
        sets.append((ref, [wide(w, 16).astype(BF16) for w in weights]))
    base = lax.broadcasted_iota(jnp.int32, (16, n), 0).astype(F32)
    zero = jnp.zeros((16, n), BF16)
    for tile in range(16):
        place = (base + float(16 * tile)).astype(BF16)
        hits = [place == key for key in keys]
        for ref, weights in sets:
            table = zero
            for m in range(3, -1, -1):
                table = jnp.where(hits[m], weights[m], table)
            ref[16 * tile : 16 * tile + 16, :] = table


def nt_dot(a, b):
    return lax.dot_general(a, b, (((1,), (1,)), ((), ())), preferred_element_type=F32)


def nn_dot(a, b):
    return lax.dot_general(a, b, (((1,), (0,)), ((), ())), preferred_element_type=F32)


def tn_dot(a, b):
    return lax.dot_general(a, b, (((0,), (0,)), ((), ())), preferred_element_type=F32)


def pair_pattern(table, pair):
    n = table.shape[1]
    iota = lax.broadcasted_iota(jnp.int32, (8, n), 0)
    return jnp.where(
        iota < 4, wide(table[2 * pair : 2 * pair + 1], 8), wide(table[2 * pair + 1 : 2 * pair + 2], 8)
    )


def spread_kernel(live_ref, charge_ref, frac_ref, cell_ref, out_ref, a_hi, a_lo, x_hi, x_lo):
    n = CHUNK
    me = lax.axis_index("gy")
    live = live_ref[0, me] * BLOCK

    def build(first, slot):
        q = charge_ref[:, pl.ds(first, n)]
        lanes = first + lax.broadcasted_iota(jnp.int32, (1, n), 1)
        q = jnp.where(lanes < live, q, 0.0)
        t = frac_ref[:, pl.ds(first, n)]
        cells = cell_ref[:, pl.ds(first, n)]
        weights = spline_weights(t)
        along = [w[2:3] * q for w in weights]
        high = [w.astype(BF16).astype(F32) for w in along]
        low = [w - h for w, h in zip(along, high)]
        x_table([(x_hi.at[slot], high), (x_lo.at[slot], low)], cells, n)
        z_main, z_halo = narrow_tables(cells, weights, 0)
        y_main, y_halo = narrow_tables(cells, weights, 1)

        def put(row, value):
            upper, lower = split(value)
            a_hi[slot, row : row + 16, :] = upper
            a_lo[slot, row : row + 16, :] = lower

        for y in range(16):
            put(16 * y, wide(y_main[y : y + 1], 16) * z_main)
        for y in range(3):
            put(320 + 16 * y, wide(y_halo[y : y + 1], 16) * z_main)
        for quad in range(4):
            put(
                256 + 16 * quad,
                jnp.concatenate(
                    [pair_pattern(y_main, 2 * quad + h) * z_halo for h in range(2)], 0
                ),
            )
        put(368, jnp.concatenate([pair_pattern(y_halo, h) * z_halo for h in range(2)], 0))

    def multiply(slot):
        out_ref[...] += (
            nt_dot(a_hi[slot], x_hi[slot])
            + nt_dot(a_hi[slot], x_lo[slot])
            + nt_dot(a_lo[slot], x_hi[slot])
        )

    out_ref[...] = jnp.zeros_like(out_ref)
    build(0, 0)

    def step(i, carry):
        build(pl.multiple_of((2 * i + 1) * n, n), 1)
        multiply(0)
        build(pl.multiple_of(lax.min(2 * i + 2, 2 * pairs - 2) * n, n), 0)
        multiply(1)
        return carry

    pairs = ATOMS_DEV // (2 * n)
    lax.fori_loop(0, pairs, step, 0)


def spread(live_blocks, charge, fractions, cells):
    return pl.pallas_call(
        spread_kernel,
        out_shape=jax.ShapeDtypeStruct((ROWS, GRID), F32),
        in_specs=[pl.BlockSpec(memory_space=pltpu.SMEM)]
        + [pl.BlockSpec(memory_space=pltpu.VMEM)] * 3,
        out_specs=pl.BlockSpec(memory_space=pltpu.VMEM),
        scratch_shapes=[
            pltpu.VMEM((2, ROWS, CHUNK), BF16),
            pltpu.VMEM((2, ROWS, CHUNK), BF16),
            pltpu.VMEM((2, GRID, CHUNK), BF16),
            pltpu.VMEM((2, GRID, CHUNK), BF16),
        ],
        name="spread",
    )(live_blocks, charge, fractions, cells)


def gather_kernel(
    live_ref, pot_ref, charge_ref, frac_ref, cell_ref, out_ref, p_hi, p_lo, w_hi, w_lo, s_hi, s_lo
):
    n = CHUNK
    me = lax.axis_index("gy")
    live = live_ref[0, me] * BLOCK
    upper, lower = split(pot_ref[...])
    p_hi[...] = upper
    p_lo[...] = lower

    def build(first, slot):
        t = frac_ref[:, pl.ds(first, n)]
        cells = cell_ref[:, pl.ds(first, n)]
        sets = []
        for values, hi_ref, lo_ref in (
            ([w[2:3] for w in spline_weights(t)], w_hi, w_lo),
            ([w[2:3] for w in spline_slopes(t)], s_hi, s_lo),
        ):
            high = [w.astype(BF16).astype(F32) for w in values]
            low = [w - h for w, h in zip(values, high)]
            sets += [(hi_ref.at[slot], high), (lo_ref.at[slot], low)]
        x_table(sets, cells, n)

    def consume(first, slot):
        q = charge_ref[:, pl.ds(first, n)]
        lanes = first + lax.broadcasted_iota(jnp.int32, (1, n), 1)
        q = jnp.where(lanes < live, q, 0.0)
        t = frac_ref[:, pl.ds(first, n)]
        cells = cell_ref[:, pl.ds(first, n)]
        weights = spline_weights(t)
        slopes = spline_slopes(t)
        zw_main, zw_halo = narrow_tables(cells, weights, 0)
        zs_main, zs_halo = narrow_tables(cells, slopes, 0)
        yw_main, yw_halo = narrow_tables(cells, weights, 1)
        ys_main, ys_halo = narrow_tables(cells, slopes, 1)
        hi, lo = p_hi[...], p_lo[...]
        along = nn_dot(hi, w_hi[slot]) + nn_dot(hi, w_lo[slot]) + nn_dot(lo, w_hi[slot])
        steep = nn_dot(hi, s_hi[slot]) + nn_dot(hi, s_lo[slot]) + nn_dot(lo, s_hi[slot])
        zero = jnp.zeros((16, n), F32)
        sums = [zero, zero, zero]
        for y in range(19):
            row = 16 * y if y < 16 else 320 + 16 * (y - 16)
            yw = wide(yw_main[y : y + 1] if y < 16 else yw_halo[y - 16 : y - 15], 16)
            ys = wide(ys_main[y : y + 1] if y < 16 else ys_halo[y - 16 : y - 15], 16)
            piece, slope = along[row : row + 16], steep[row : row + 16]
            sums = [sums[0] + yw * piece, sums[1] + ys * piece, sums[2] + yw * slope]
        zero = jnp.zeros((8, n), F32)
        rims = [zero, zero, zero]
        for pair in range(10):
            row = 256 + 8 * pair if pair < 8 else 368 + 8 * (pair - 8)
            yw = pair_pattern(yw_main, pair) if pair < 8 else pair_pattern(yw_halo, pair - 8)
            ys = pair_pattern(ys_main, pair) if pair < 8 else pair_pattern(ys_halo, pair - 8)
            piece, slope = along[row : row + 8], steep[row : row + 8]
            rims = [rims[0] + yw * piece, rims[1] + ys * piece, rims[2] + yw * slope]
        force_z = sums[0] * zs_main
        force_y = sums[1] * zw_main
        force_x = sums[2] * zw_main
        force_z = force_z[:8] + force_z[8:] + rims[0] * zs_halo
        force_y = force_y[:8] + force_y[8:] + rims[1] * zw_halo
        force_x = force_x[:8] + force_x[8:] + rims[2] * zw_halo
        result = [jnp.sum(f, axis=0, keepdims=True) * -q for f in (force_z, force_y, force_x)]
        out_ref[:, pl.ds(first, n)] = jnp.concatenate(result, 0)

    build(0, 0)
    pairs = ATOMS_DEV // (2 * n)

    def step(i, carry):
        first = pl.multiple_of(2 * i * n, n)
        second = pl.multiple_of((2 * i + 1) * n, n)
        build(second, 1)
        consume(first, 0)
        build(pl.multiple_of(lax.min(2 * i + 2, 2 * pairs - 2) * n, n), 0)
        consume(second, 1)
        return carry

    lax.fori_loop(0, pairs, step, 0)


def gather(live_blocks, potential, charge, fractions, cells):
    return pl.pallas_call(
        gather_kernel,
        out_shape=jax.ShapeDtypeStruct((3, ATOMS_DEV), F32),
        in_specs=[pl.BlockSpec(memory_space=pltpu.SMEM)]
        + [pl.BlockSpec(memory_space=pltpu.VMEM)] * 4,
        out_specs=pl.BlockSpec(memory_space=pltpu.VMEM),
        scratch_shapes=[
            pltpu.VMEM((ROWS, GRID), BF16),
            pltpu.VMEM((ROWS, GRID), BF16),
        ]
        + [pltpu.VMEM((2, GRID, CHUNK), BF16)] * 4,
        name="gather",
    )(live_blocks, potential, charge, fractions, cells)


def turn(arrays):
    arrays = list(arrays)
    rows = arrays[0].shape[0]
    group = lax.broadcasted_iota(jnp.int32, (rows, 128), 1) >> 3
    for bit in range(4):
        g = 1 << bit
        keep = (group & g) == 0
        fresh = list(arrays)
        for i in range(16):
            if i & g == 0:
                low, high = arrays[i], arrays[i | g]
                fresh[i] = jnp.where(keep, low, pltpu.roll(high, 8 * g, 1))
                fresh[i | g] = jnp.where(keep, pltpu.roll(low, 128 - 8 * g, 1), high)
        arrays = fresh
    return arrays


def tables_of_influence(moduli_ref, screening, a, b):
    m = [moduli_ref[c : c + 1, :] for c in range(3)]
    lane_k = lax.broadcasted_iota(jnp.int32, (256, 256), 1)
    row_k = lax.broadcasted_iota(jnp.int32, (256, 256), 0)
    same = lane_k == row_k
    other = lane_k == ((256 - row_k) & 255)

    def column(row, mask):
        return jnp.sum(jnp.where(mask, wide(row, 256), 0.0), axis=1, keepdims=True)

    m0, m1, m2 = column(m[0], same), column(m[1], same), column(m[2], same)
    m1_back = column(m[1], other)

    lane = lax.broadcasted_iota(jnp.int32, (1, 128), 1)
    local, j = lane >> 3, lane & 7
    step = 8 * b + (local >> 1)
    kz = jnp.where(local & 1 == 0, step, jnp.where(step == 0, 128, 256 - step))
    kx = 8 * a + j
    rows = lax.broadcasted_iota(jnp.int32, (256, 128), 0)

    def along_lanes(col, index):
        hit = rows == wide(index, 256)
        return jnp.sum(jnp.where(hit, jnp.broadcast_to(col, (256, 128)), 0.0), 0, keepdims=True)

    z0, z1 = along_lanes(m0, kz), along_lanes(m0, (256 - kz) & 255)
    x0, x1 = along_lanes(m2, kx), along_lanes(m2, (256 - kx) & 255)
    xn = along_lanes(m2, jnp.full_like(kx, 128))

    def signed(k):
        return jnp.where(k < 128, k, k - 256)

    nz, ny = signed(kz), signed(rows)
    flat = ny * ny + wide(nz * nz, 256)

    def kernel_at(nx, first, second):
        radius = flat + wide(nx * nx, 256)
        squared = radius.astype(F32) / float(GRID * GRID)
        safe = jnp.where(radius > 0, squared, 1.0)
        product = m1 * wide(z0 * first, 256) + m1_back * wide(z1 * second, 256)
        return jnp.where(radius > 0, product * jnp.exp(-screening * squared) / safe, 0.0)

    at_kx = kernel_at(kx, x0, x1)
    at_last = kernel_at(jnp.full_like(kx, 128), xn, xn)
    packed = (rows >= 0) & wide(kx == 0, 256)
    straight = jnp.where(packed, 0.5 * (at_kx + at_last), at_kx)
    crossed = jnp.where(packed, 0.5 * (at_kx - at_last), 0.0)
    return straight, crossed


def solve_kernel(
    screening_ref,
    tile_ref,
    moduli_ref,
    fx_hi,
    fx_lo,
    gx_hi,
    gx_lo,
    fz_hi,
    fz_lo,
    fy_hi,
    fy_lo,
    out_ref,
    rim_in,
    send_1,
    recv_1,
    send_2,
    recv_2,
    send_3,
    recv_3,
    send_4,
    recv_4,
    straight_ref,
    crossed_ref,
    work,
    rim_sems,
    send_sems,
    recv_sems,
):
    a, b = lax.axis_index("gz"), lax.axis_index("gy")
    barrier = pltpu.get_barrier_semaphore()

    def greet(s, carry):
        pl.semaphore_signal(
            barrier, inc=1, device_id=((a + s) & 15, b), device_id_type=MESH
        )
        pl.semaphore_signal(
            barrier, inc=1, device_id=(a, (b + s) & 15), device_id_type=MESH
        )
        return carry

    lax.fori_loop(1, NPEER, greet, 0)
    pl.semaphore_wait(barrier, 2 * (NPEER - 1))

    def exchange(stage, src, dst, size, over_z):
        me = a if over_z else b

        def copy(peer, slot):
            return pltpu.make_async_remote_copy(
                src_ref=src.at[pl.ds(pl.multiple_of(peer * size, size), size), :],
                dst_ref=dst.at[pl.ds(pl.multiple_of(slot * size, size), size), :],
                send_sem=send_sems.at[stage, peer],
                recv_sem=recv_sems.at[stage, slot],
                device_id=(peer, b) if over_z else (a, peer),
                device_id_type=MESH,
            )

        def start(s, carry):
            copy((me + s) & 15, me).start()
            return carry

        def arrive(s, carry):
            peer = (me + s) & 15
            copy(peer, peer).wait_recv()
            return carry

        def leave(s, carry):
            copy((me + s) & 15, me).wait_send()
            return carry

        lax.fori_loop(1, NPEER, start, 0)
        own = pl.ds(pl.multiple_of(me * size, size), size)
        dst[own, :] = src[own, :]
        return (
            lambda: lax.fori_loop(1, NPEER, arrive, 0),
            lambda: lax.fori_loop(1, NPEER, leave, 0),
        )

    rim = pltpu.make_async_remote_copy(
        src_ref=tile_ref.at[pl.ds(320, 64), :],
        dst_ref=rim_in,
        send_sem=rim_sems.at[0],
        recv_sem=rim_sems.at[1],
        device_id=(a, (b + 1) & 15),
        device_id_type=MESH,
    )
    rim.start()
    straight, crossed = tables_of_influence(moduli_ref, screening_ref[0], a, b)
    straight_ref[...] = straight
    crossed_ref[...] = crossed
    rim.wait()
    work[...] = tile_ref[:320, :]
    work[0:48, :] += rim_in[0:48, :]
    work[256:272, :] += rim_in[48:64, :]

    high, low = split(work[...])
    spectrum = nn_dot(high, fx_hi[...]) + nn_dot(high, fx_lo[...]) + nn_dot(low, fx_hi[...])
    iota = lax.broadcasted_iota(jnp.int32, (8, 128), 0)
    pieces = []
    for y in range(16):
        real = spectrum[16 * y : 16 * y + 16, :128]
        imag = spectrum[16 * y : 16 * y + 16, 128:]
        row = 256 + 8 * (y // 2)
        rim_real, rim_imag = spectrum[row : row + 8, :128], spectrum[row : row + 8, 128:]
        if y % 2 == 0:
            halo = jnp.where(iota < 4, rim_real, pltpu.roll(rim_imag, 4, 0))
        else:
            halo = jnp.where(iota < 4, pltpu.roll(rim_real, 4, 0), rim_imag)
        pieces.append(jnp.concatenate([real, imag, halo], 0))
    for peer, piece in enumerate(turn(pieces)):
        send_1[MSG_Z * peer : MSG_Z * peer + MSG_Z, :] = piece
    arrive, leave_1 = exchange(0, send_1, recv_1, MSG_Z, True)
    arrive()

    high, low = split(recv_1[...])
    both = nn_dot(fz_hi[...], jnp.concatenate([high, low], 1))
    waves = both[:, :128] + both[:, 128:] + nn_dot(fz_lo[...], high)
    turned = turn([waves[32 * k : 32 * k + 32] for k in range(16)])
    for y in range(16):
        for c in range(2):
            send_2[pl.ds(16 * c + y, 16, stride=32), :] = turned[y][16 * c : 16 * c + 16]
    arrive, leave_2 = exchange(1, send_2, recv_2, MSG_Y, False)
    arrive()

    lines = recv_2[...]
    lane = lax.broadcasted_iota(jnp.int32, (512, 128), 1)
    row = lax.broadcasted_iota(jnp.int32, (512, 128), 0)
    odd = (lane >> 3) & 1
    swapped = jnp.where(odd == 0, pltpu.roll(lines, 120, 1), pltpu.roll(lines, 8, 1))
    swapped = jnp.where((lane < 16 * (b == 0).astype(jnp.int32)), lines, swapped)
    swapped = jnp.where((row >> 4) & 1 == 0, swapped, -swapped)
    high, low = split(jnp.concatenate([lines, swapped], 1))
    waves = nn_dot(fy_hi[...], high) + nn_dot(fy_hi[...], low) + nn_dot(fy_lo[...], high)
    straight = jnp.concatenate([straight_ref[...]] * 2, 0)
    crossed = jnp.concatenate([crossed_ref[...]] * 2, 0)
    high, low = split(waves[:, :128] * straight + waves[:, 128:] * crossed)
    both = tn_dot(fy_hi[...], jnp.concatenate([high, low], 1))
    send_3[...] = (both[:, :128] + both[:, 128:] + tn_dot(fy_lo[...], high)) * (1.0 / 256)
    arrive, leave_3 = exchange(2, send_3, recv_3, MSG_Y, False)
    arrive()

    pieces = []
    for y in range(16):
        pieces.append(
            jnp.concatenate(
                [recv_3[pl.ds(16 * c + y, 16, stride=32), :] for c in range(2)], 0
            )
        )
    high, low = split(jnp.concatenate(turn(pieces), 0))
    both = tn_dot(fz_hi[...], jnp.concatenate([high, low], 1))
    send_4[...] = (both[:, :128] + both[:, 128:] + tn_dot(fz_lo[...], high)) * (1.0 / 256)
    arrive, leave_4 = exchange(3, send_4, recv_4, MSG_Z, True)
    arrive()

    turned = turn([recv_4[MSG_Z * k : MSG_Z * k + MSG_Z, :] for k in range(16)])
    lines = [jnp.concatenate([t[0:16], t[16:32]], 1) for t in turned]
    for pair in range(8):
        even, odd = turned[2 * pair][32:40], turned[2 * pair + 1][32:40]
        real = jnp.where(iota < 4, even, pltpu.roll(odd, 4, 0))
        imag = jnp.where(iota < 4, pltpu.roll(even, 4, 0), odd)
        lines.append(jnp.concatenate([real, imag], 1))
    high, low = split(jnp.concatenate(lines, 0))
    out_ref[0:320, :] = (
        nn_dot(high, gx_hi[...]) + nn_dot(high, gx_lo[...]) + nn_dot(low, gx_hi[...])
    )

    rims = [
        pltpu.make_async_remote_copy(
            src_ref=out_ref.at[pl.ds(source, size), :],
            dst_ref=out_ref.at[pl.ds(target, size), :],
            send_sem=rim_sems.at[2 + 2 * k],
            recv_sem=rim_sems.at[3 + 2 * k],
            device_id=(a, (b + 15) & 15),
            device_id_type=MESH,
        )
        for k, (source, target, size) in enumerate(((0, 320, 48), (256, 368, 16)))
    ]
    for copy in rims:
        copy.start()
    leave_1()
    leave_2()
    leave_3()
    leave_4()
    for copy in rims:
        copy.wait()


def solve(tile, moduli, screening):
    tables = []
    for table in (forward_x(), inverse_x(), forward_z(), forward_y()):
        tables += [jnp.asarray(part) for part in split_np(table)]
    message_z = pltpu.VMEM((NPEER * MSG_Z, 128), F32)
    message_y = pltpu.VMEM((NPEER * MSG_Y, 128), F32)
    return pl.pallas_call(
        solve_kernel,
        out_shape=jax.ShapeDtypeStruct((ROWS, GRID), F32),
        in_specs=[pl.BlockSpec(memory_space=pltpu.SMEM)]
        + [pl.BlockSpec(memory_space=pltpu.VMEM)] * (2 + len(tables)),
        out_specs=pl.BlockSpec(memory_space=pltpu.VMEM),
        scratch_shapes=[pltpu.VMEM((64, GRID), F32)]
        + [message_z] * 2
        + [message_y] * 4
        + [message_z] * 2
        + [pltpu.VMEM((256, 128), F32)] * 2
        + [
            pltpu.VMEM((320, GRID), F32),
            pltpu.SemaphoreType.DMA((6,)),
            pltpu.SemaphoreType.DMA((4, NPEER)),
            pltpu.SemaphoreType.DMA((4, NPEER)),
        ],
        compiler_params=pltpu.CompilerParams(collective_id=0, has_side_effects=True),
        name="solve",
    )(screening, tile, moduli, *tables)


def body(charge, fractions, cell_base, live_blocks, send_blocks, moduli, screening):
    column = lax.axis_index("gy")
    before = (column + NPEER - 1) % NPEER
    lanes = lax.iota(jnp.int32, NPEER)

    def pick(table, index):
        return jnp.sum(jnp.where(lanes == index, table[0], 0))

    kept = (pick(live_blocks, column) - pick(send_blocks, column)) * BLOCK
    arriving = pick(send_blocks, before) * BLOCK

    charge = charge[None, :]
    tile = spread(live_blocks, charge, fractions, cell_base)
    potential = solve(tile, moduli, screening)
    home = gather(live_blocks, potential, charge, fractions, cell_base)

    margin = SEND_MAX * BLOCK
    padded = jnp.concatenate([home, jnp.zeros((3, margin), F32)], 1)
    lent = lax.dynamic_slice_in_dim(padded, kept, margin, 1)
    guests = lax.ppermute(lent, "gy", [(i, (i + 1) % NPEER) for i in range(NPEER)])
    places = lax.iota(jnp.int32, margin)
    guests = jnp.where(places < arriving, guests, 0.0)
    slots = lax.iota(jnp.int32, ATOMS_DEV + margin)
    own = jnp.where(slots < kept, padded, 0.0)
    return lax.dynamic_update_slice_in_dim(own, guests, kept, 1)[:, :ATOMS_DEV]


def solution(mesh):
    return jax.shard_map(
        body,
        mesh=mesh,
        in_specs=(
            P(("gz", "gy")),
            P(None, ("gz", "gy")),
            P(None, ("gz", "gy")),
            P("gz", None),
            P("gz", None),
            P(),
            P(),
        ),
        out_specs=P(None, ("gz", "gy")),
        check_vma=False,
    )
```

```python
import functools

import jax
import jax.numpy as jnp
import numpy as np
from jax import lax
from jax.experimental import pallas as pl
from jax.experimental.pallas import tpu as pltpu
from jax.sharding import PartitionSpec as P

GRID = 256
BLOCK = 128
ATOMS_DEV = 12288
NBLK = 96
SEND_MAX = 36
NPEER = 16
CHUNK = 512
SPREAD_UNROLL = 4
GATHER_UNROLL = 3
ROWS = 384
MSG_Z = 40
MSG_Y = 32
MESH = pl.DeviceIdType.MESH
BF16 = jnp.bfloat16
F32 = jnp.float32


def split_np(table):
    table = np.asarray(table, np.float32)
    high = table.astype(jnp.bfloat16)
    low = (table - high.astype(np.float32)).astype(jnp.bfloat16)
    return high, low


def kz_of(block, local):
    j = 8 * block + local // 2
    return np.where(local % 2 == 0, j, np.where(j == 0, 128, (256 - j) % 256))


def forward_x():
    x = np.arange(256)[:, None]
    k = np.arange(128)[None, :]
    angle = 2 * np.pi * ((x * k) % 256) / 256
    table = np.concatenate([np.cos(angle), -np.sin(angle)], 1)
    table[:, 128] = (-1.0) ** np.arange(256)
    return table


def inverse_x():
    k = np.arange(128)[:, None]
    x = np.arange(256)[None, :]
    angle = 2 * np.pi * ((x * k) % 256) / 256
    table = np.concatenate([2 * np.cos(angle), -2 * np.sin(angle)], 0) / 256
    table[0] = 1.0 / 256
    table[128] = (-1.0) ** np.arange(256) / 256
    return table


def message_rows_z():
    part = np.zeros(MSG_Z, np.int64)
    place = np.zeros(MSG_Z, np.int64)
    for c in range(2):
        part[16 * c : 16 * c + 16] = c
        place[16 * c : 16 * c + 16] = np.arange(16)
        part[32 + 4 * c : 36 + 4 * c] = c
        place[32 + 4 * c : 36 + 4 * c] = 16 + np.arange(4)
    return part, place


def complex_table(part_out, wave, part_in, place):
    angle = 2 * np.pi * ((wave[:, None] * place[None, :]) % 256) / 256
    cosine, sine = np.cos(angle), np.sin(angle)
    same = part_out[:, None] == part_in[None, :]
    sign = np.where(part_out[:, None] == 0, 1.0, -1.0)
    return np.where(same, cosine, sign * sine)


def forward_z():
    local, part, block = np.meshgrid(np.arange(16), np.arange(2), np.arange(16), indexing="ij")
    wave = kz_of(block, local).reshape(-1)
    part = part.reshape(-1)
    part_in, place = message_rows_z()
    place_all = (16 * np.arange(16)[:, None] + place[None, :]).reshape(-1)
    table = complex_table(part, wave, np.tile(part_in, 16), place_all)
    pad = np.tile(place == 19, 16)
    return np.where(pad[None, :], 0.0, table)


def forward_y():
    part, wave = np.meshgrid(np.arange(2), np.arange(256), indexing="ij")
    block, part_in, place = np.meshgrid(np.arange(16), np.arange(2), np.arange(16), indexing="ij")
    return complex_table(
        part.reshape(-1), wave.reshape(-1), part_in.reshape(-1), (16 * block + place).reshape(-1)
    )


def split(value):
    high = value.astype(BF16)
    low = (value - high.astype(F32)).astype(BF16)
    return high, low


def spline_weights(t):
    remain = 1.0 - t
    square = t * t
    cubed = square * t
    sixth = 1.0 / 6.0
    weights = [
        remain * remain * remain * sixth,
        (3.0 * cubed - 6.0 * square + 4.0) * sixth,
        (-3.0 * cubed + 3.0 * square + 3.0 * t + 1.0) * sixth,
        cubed * sixth,
    ]
    return weights


def spline_slopes(t):
    remain = 1.0 - t
    square = t * t
    return [
        -0.5 * remain * remain,
        1.5 * square - 2.0 * t,
        -1.5 * square + t + 0.5,
        0.5 * square,
    ]


def wide(row, count):
    return jnp.broadcast_to(row, (count, row.shape[1]))


def stencil(offset, cell, weights):
    rows = offset.shape[0]
    place = offset - wide(cell, rows)
    table = jnp.zeros(offset.shape, F32)
    for k in range(3, -1, -1):
        table = jnp.where(place == k, wide(weights[k], rows), table)
    return table


def narrow_tables(cells, weights, row):
    cell = cells[row : row + 1]
    picked = [w[row : row + 1] for w in weights]
    iota = lax.broadcasted_iota(jnp.int32, (16, cell.shape[1]), 0)
    return stencil(iota, cell, picked), stencil(16 + (iota[:8] & 3), cell, picked)


def x_tables(cells, weight_sets):
    cell = cells[2:3]
    keys = [wide(((cell + m) & 255).astype(F32), 16).astype(BF16) for m in range(4)]
    sets = [[wide(w, 16).astype(BF16) for w in weights] for weights in weight_sets]
    base = lax.broadcasted_iota(jnp.int32, (16, 128), 0).astype(F32)
    results = [[] for _ in sets]
    for tile in range(16):
        place = (base + float(16 * tile)).astype(BF16)
        tables = [jnp.zeros((16, 128), BF16) for _ in sets]
        for m in range(3, -1, -1):
            hit = place == keys[m]
            tables = [jnp.where(hit, weights[m], t) for weights, t in zip(sets, tables)]
        for result, table in zip(results, tables):
            result.append(table)
    return [jnp.concatenate(result, 0) for result in results]


def high_low(rows):
    high = [w.astype(BF16).astype(F32) for w in rows]
    return high, [w - h for w, h in zip(rows, high)]


def nt_dot(a, b):
    return lax.dot_general(a, b, (((1,), (1,)), ((), ())), preferred_element_type=F32)


def nn_dot(a, b):
    return lax.dot_general(a, b, (((1,), (0,)), ((), ())), preferred_element_type=F32)


def tn_dot(a, b):
    return lax.dot_general(a, b, (((0,), (0,)), ((), ())), preferred_element_type=F32)


def pair_pattern(table, pair):
    iota = lax.broadcasted_iota(jnp.int32, (8, table.shape[1]), 0)
    return jnp.where(
        iota < 4, wide(table[2 * pair : 2 * pair + 1], 8), wide(table[2 * pair + 1 : 2 * pair + 2], 8)
    )


def plane_tables(cells, weights):
    z_main, z_halo = narrow_tables(cells, weights, 0)
    y_main, y_halo = narrow_tables(cells, weights, 1)
    pieces = [wide(y_main[y : y + 1], 16) * z_main for y in range(16)]
    pieces += [pair_pattern(y_main, pair) * z_halo for pair in range(8)]
    pieces += [wide(y_halo[y : y + 1], 16) * z_main for y in range(3)]
    pieces += [pair_pattern(y_halo, pair) * z_halo for pair in range(2)]
    return split(jnp.concatenate(pieces, 0))


def spread_atoms(live, charge_ref, frac_ref, cell_ref, tile_ref):
    n = CHUNK
    tile_ref[...] = jnp.zeros_like(tile_ref)

    def chunk(first):
        q_all = charge_ref[:, pl.ds(first, n)]
        lanes = first + lax.broadcasted_iota(jnp.int32, (1, n), 1)
        q_all = jnp.where(lanes < live, q_all, 0.0)
        weights_all = spline_weights(frac_ref[:, pl.ds(first, n)])
        cells_all = cell_ref[:, pl.ds(first, n)]
        columns = []
        for group in range(n // 128):
            lanes = slice(128 * group, 128 * group + 128)
            weights = [w[:, lanes] for w in weights_all]
            cells, q = cells_all[:, lanes], q_all[:, lanes]
            columns.append(
                tuple(x_tables(cells, high_low([w[2:3] * q for w in weights])))
                + plane_tables(cells, weights)
            )
        x_hi, x_lo, a_hi, a_lo = (jnp.concatenate(part, 1) for part in zip(*columns))
        tile_ref[...] += nt_dot(a_hi, x_hi) + nt_dot(a_hi, x_lo) + nt_dot(a_lo, x_hi)

    def step(i, carry):
        for u in range(SPREAD_UNROLL):
            chunk(pl.multiple_of((SPREAD_UNROLL * i + u) * n, n))
        return carry

    lax.fori_loop(0, ATOMS_DEV // (n * SPREAD_UNROLL), step, 0)


def gather_atoms(chunks, charge_ref, frac_ref, cell_ref, out_ref, p_hi, p_lo):
    n = 256

    def piece_of(first):
        t = frac_ref[:, pl.ds(first, n)]
        cells_all = cell_ref[:, pl.ds(first, n)]
        weights_all, slopes_all = spline_weights(t), spline_slopes(t)
        columns = []
        for group in range(n // 128):
            lanes = slice(128 * group, 128 * group + 128)
            columns.append(
                x_tables(
                    cells_all[:, lanes],
                    high_low([w[2:3, lanes] for w in weights_all])
                    + high_low([w[2:3, lanes] for w in slopes_all]),
                )
            )
        w_hi, w_lo, s_hi, s_lo = (jnp.concatenate(part, 1) for part in zip(*columns))
        hi, lo = p_hi[...], p_lo[...]
        along_all = nn_dot(hi, w_hi) + nn_dot(hi, w_lo) + nn_dot(lo, w_hi)
        steep_all = nn_dot(hi, s_hi) + nn_dot(hi, s_lo) + nn_dot(lo, s_hi)
        results = []
        for group in range(n // 128):
            lanes = slice(128 * group, 128 * group + 128)
            along, steep = along_all[:, lanes], steep_all[:, lanes]
            weights = [w[:, lanes] for w in weights_all]
            slopes = [w[:, lanes] for w in slopes_all]
            cells = cells_all[:, lanes]
            zw_main, zw_halo = narrow_tables(cells, weights, 0)
            zs_main, zs_halo = narrow_tables(cells, slopes, 0)
            yw_main, yw_halo = narrow_tables(cells, weights, 1)
            ys_main, ys_halo = narrow_tables(cells, slopes, 1)
            sums = [jnp.zeros((16, 128), F32)] * 3
            for y in range(19):
                row = 16 * y if y < 16 else 320 + 16 * (y - 16)
                yw = wide(yw_main[y : y + 1] if y < 16 else yw_halo[y - 16 : y - 15], 16)
                ys = wide(ys_main[y : y + 1] if y < 16 else ys_halo[y - 16 : y - 15], 16)
                piece, slope = along[row : row + 16], steep[row : row + 16]
                sums = [sums[0] + yw * piece, sums[1] + ys * piece, sums[2] + yw * slope]
            rims = [jnp.zeros((8, 128), F32)] * 3
            for pair in range(10):
                row = 256 + 8 * pair if pair < 8 else 368 + 8 * (pair - 8)
                yw = pair_pattern(yw_main, pair) if pair < 8 else pair_pattern(yw_halo, pair - 8)
                ys = pair_pattern(ys_main, pair) if pair < 8 else pair_pattern(ys_halo, pair - 8)
                piece, slope = along[row : row + 8], steep[row : row + 8]
                rims = [rims[0] + yw * piece, rims[1] + ys * piece, rims[2] + yw * slope]
            sums = [sums[0] * zs_main, sums[1] * zw_main, sums[2] * zw_main]
            rims = [rims[0] * zs_halo, rims[1] * zw_halo, rims[2] * zw_halo]
            results.append(
                jnp.concatenate(
                    [
                        jnp.sum(f[:8] + f[8:] + r, axis=0, keepdims=True)
                        for f, r in zip(sums, rims)
                    ],
                    0,
                )
            )
        q = charge_ref[:, pl.ds(first, n)]
        out_ref[:, pl.ds(first, n)] = jnp.concatenate(results, 1) * -q

    low, high = chunks
    per_step = GATHER_UNROLL * CHUNK

    def step(i, carry):
        for u in range(per_step // n):
            piece_of(pl.multiple_of(low * CHUNK + i * per_step + u * n, n))
        return carry

    lax.fori_loop(0, (high - low) // GATHER_UNROLL, step, 0)


def turn(arrays):
    arrays = list(arrays)
    rows = arrays[0].shape[0]
    group = lax.broadcasted_iota(jnp.int32, (rows, 128), 1) >> 3
    for bit in range(4):
        g = 1 << bit
        keep = (group & g) == 0
        fresh = list(arrays)
        for i in range(16):
            if i & g == 0:
                low, high = arrays[i], arrays[i | g]
                fresh[i] = jnp.where(keep, low, pltpu.roll(high, 8 * g, 1))
                fresh[i | g] = jnp.where(keep, pltpu.roll(low, 128 - 8 * g, 1), high)
        arrays = fresh
    return arrays


def tables_of_influence(moduli_ref, screening, a, b):
    m = [moduli_ref[c : c + 1, :] for c in range(3)]
    lane_k = lax.broadcasted_iota(jnp.int32, (256, 256), 1)
    row_k = lax.broadcasted_iota(jnp.int32, (256, 256), 0)
    same = lane_k == row_k
    other = lane_k == ((256 - row_k) & 255)

    def column(row, mask):
        return jnp.sum(jnp.where(mask, wide(row, 256), 0.0), axis=1, keepdims=True)

    m0, m1, m2 = column(m[0], same), column(m[1], same), column(m[2], same)
    m1_back = column(m[1], other)

    lane = lax.broadcasted_iota(jnp.int32, (1, 128), 1)
    local, j = lane >> 3, lane & 7
    step = 8 * b + (local >> 1)
    kz = jnp.where(local & 1 == 0, step, jnp.where(step == 0, 128, 256 - step))
    kx = 8 * a + j
    rows = lax.broadcasted_iota(jnp.int32, (256, 128), 0)

    def along_lanes(col, index):
        hit = rows == wide(index, 256)
        return jnp.sum(jnp.where(hit, jnp.broadcast_to(col, (256, 128)), 0.0), 0, keepdims=True)

    z0, z1 = along_lanes(m0, kz), along_lanes(m0, (256 - kz) & 255)
    x0, x1 = along_lanes(m2, kx), along_lanes(m2, (256 - kx) & 255)
    xn = along_lanes(m2, jnp.full_like(kx, 128))

    def signed(k):
        return jnp.where(k < 128, k, k - 256)

    nz, ny = signed(kz), signed(rows)
    flat = ny * ny + wide(nz * nz, 256)

    def kernel_at(nx, first, second):
        radius = flat + wide(nx * nx, 256)
        squared = radius.astype(F32) / float(GRID * GRID)
        safe = jnp.where(radius > 0, squared, 1.0)
        product = m1 * wide(z0 * first, 256) + m1_back * wide(z1 * second, 256)
        return jnp.where(radius > 0, product * jnp.exp(-screening * squared) / safe, 0.0)

    at_kx = kernel_at(kx, x0, x1)
    at_last = kernel_at(jnp.full_like(kx, 128), xn, xn)
    packed = (rows >= 0) & wide(kx == 0, 256)
    straight = jnp.where(packed, 0.5 * (at_kx + at_last), at_kx)
    crossed = jnp.where(packed, 0.5 * (at_kx - at_last), 0.0)
    return straight, crossed


def block(ref, index):
    return ref[:, BLOCK * index : BLOCK * index + BLOCK]


def shift_left(blocks, amount, top, keep):
    bit = top
    while bit:
        take = wide((amount & bit) > 0, blocks[0].shape[0])
        count = min(len(blocks), keep + bit - 1)
        last = len(blocks) - 1
        blocks = [
            jnp.where(take, blocks[min(i + bit, last)], blocks[i]) for i in range(count)
        ]
        bit //= 2
    return blocks


def handed_first(live, kept, charge_ref, frac_ref, cell_ref, charge_out, frac_out, cell_out):
    home = NBLK - SEND_MAX
    start = jnp.minimum(jnp.full((1, BLOCK), kept, jnp.int32), home)
    count = jnp.full((1, BLOCK), live, jnp.int32)
    charges = [jnp.where(count > i, block(charge_ref, i), 0.0) for i in range(NBLK)]
    for blocks, out in (
        (charges, charge_out),
        ([block(frac_ref, i) for i in range(NBLK)], frac_out),
        ([block(cell_ref, i) for i in range(NBLK)], cell_out),
    ):
        ordered = shift_left(blocks, start, 32, SEND_MAX) + blocks[:home]
        for i, value in enumerate(ordered):
            out[:, BLOCK * i : BLOCK * i + BLOCK] = value


def place_forces(kept, kept_before, arriving, forces, guests, out_ref):
    home = NBLK - SEND_MAX
    kept = jnp.full((1, BLOCK), kept, jnp.int32)
    kept_before = jnp.full((1, BLOCK), kept_before, jnp.int32)
    end = kept + arriving
    skip = kept_before - jnp.minimum(kept_before, home)
    arrived = shift_left([block(guests, i) for i in range(SEND_MAX)], skip, 32, SEND_MAX)
    placed = arrived + [jnp.zeros((3, BLOCK), F32)] * (NBLK - SEND_MAX)
    bit = 64
    while bit:
        take = wide((kept & bit) > 0, 3)
        placed = [
            jnp.where(take, placed[i - bit] if i >= bit else 0.0, placed[i]) for i in range(NBLK)
        ]
        bit //= 2
    for slot in range(NBLK):
        own = block(forces, SEND_MAX + slot if slot < home else slot - home)
        guest = jnp.where(wide(end > slot, 3), placed[slot], 0.0)
        out_ref[:, BLOCK * slot : BLOCK * slot + BLOCK] = jnp.where(wide(kept > slot, 3), own, guest)


def offsets_z():
    return [(dz, dy) for dz in (4, 3, -3, 2, -2, 1, -1, 0) for dy in (1, 0) if (dz, dy) != (0, 0)]


def offsets_y():
    moves = [(dx, dy, dc) for dx in (2, 1, -1, 0) for dy in (1, 0) for dc in (1, 0)]
    moves.remove((0, 0, 0))
    return sorted(moves, key=lambda m: -(abs(m[0]) + 2 * m[1]))


def solve_kernel(
    live_ref,
    send_ref,
    screening_ref,
    charge_ref,
    frac_ref,
    cell_ref,
    moduli_ref,
    fx_hi,
    fx_lo,
    gx_hi,
    gx_lo,
    fz_hi,
    fz_lo,
    fy_hi,
    fy_lo,
    out_ref,
    tile_ref,
    pot_ref,
    rim_in,
    send_1,
    recv_1,
    send_2,
    recv_2,
    send_3,
    recv_3,
    send_4,
    recv_4,
    straight_ref,
    crossed_ref,
    work,
    p_hi,
    p_lo,
    forces,
    guests,
    charge_in_order,
    frac_in_order,
    cell_in_order,
    rim_sems,
    send_sems,
    recv_sems,
):
    a, b = lax.axis_index("gz"), lax.axis_index("gy")
    barrier = pltpu.get_barrier_semaphore()
    peers_z = [
        ((a // 2 + dz + 8) % 8) * 2 + (a + dy) % 2 for dz, dy in offsets_z()
    ]
    peers_y = [
        ((b // 4 + dx + 4) % 4) * 4 + ((b // 2 + dy) % 2) * 2 + (b + dc) % 2
        for dx, dy, dc in offsets_y()
    ]
    for peer in peers_z:
        pl.semaphore_signal(barrier, inc=1, device_id=(peer, b), device_id_type=MESH)
    for peer in peers_y:
        pl.semaphore_signal(barrier, inc=1, device_id=(a, peer), device_id_type=MESH)

    before = (b + 15) % 16
    live = live_ref[0, b]
    kept = live - send_ref[0, b]
    kept_before = live_ref[0, before] - send_ref[0, before]
    arriving = send_ref[0, before]
    spread_atoms(live * BLOCK, charge_ref, frac_ref, cell_ref, tile_ref)
    pl.semaphore_wait(barrier, 2 * (NPEER - 1))

    def exchange(stage, src, dst, size, over_z):
        me = a if over_z else b
        peers = peers_z if over_z else peers_y

        def copy(peer, slot):
            return pltpu.make_async_remote_copy(
                src_ref=src.at[pl.ds(pl.multiple_of(peer * size, 8), size), :],
                dst_ref=dst.at[pl.ds(pl.multiple_of(slot * size, 8), size), :],
                send_sem=send_sems.at[stage, peer],
                recv_sem=recv_sems.at[stage, slot],
                device_id=(peer, b) if over_z else (a, peer),
                device_id_type=MESH,
            )

        for peer in peers:
            copy(peer, me).start()
        own = pl.ds(pl.multiple_of(me * size, 8), size)
        dst[own, :] = src[own, :]

        def arrive():
            for peer in peers:
                copy(peer, peer).wait_recv()

        def leave():
            for peer in peers:
                copy(peer, me).wait_send()

        return arrive, leave

    rim = pltpu.make_async_remote_copy(
        src_ref=tile_ref.at[pl.ds(320, 64), :],
        dst_ref=rim_in,
        send_sem=rim_sems.at[0],
        recv_sem=rim_sems.at[1],
        device_id=(a, (b + 1) % 16),
        device_id_type=MESH,
    )
    rim.start()
    rim.wait()
    work[...] = tile_ref[:320, :]
    work[0:48, :] += rim_in[0:48, :]
    work[256:272, :] += rim_in[48:64, :]

    high, low = split(work[...])
    spectrum = nn_dot(high, fx_hi[...]) + nn_dot(high, fx_lo[...]) + nn_dot(low, fx_hi[...])
    iota = lax.broadcasted_iota(jnp.int32, (8, 128), 0)
    pieces = []
    for y in range(16):
        real = spectrum[16 * y : 16 * y + 16, :128]
        imag = spectrum[16 * y : 16 * y + 16, 128:]
        row = 256 + 8 * (y // 2)
        rim_real, rim_imag = spectrum[row : row + 8, :128], spectrum[row : row + 8, 128:]
        if y % 2 == 0:
            halo = jnp.where(iota < 4, rim_real, pltpu.roll(rim_imag, 4, 0))
        else:
            halo = jnp.where(iota < 4, pltpu.roll(rim_real, 4, 0), rim_imag)
        pieces.append(jnp.concatenate([real, imag, halo], 0))
    for peer, piece in enumerate(turn(pieces)):
        send_1[MSG_Z * peer : MSG_Z * peer + MSG_Z, :] = piece
    arrive, leave_1 = exchange(0, send_1, recv_1, MSG_Z, True)
    straight, crossed = tables_of_influence(moduli_ref, screening_ref[0], a, b)
    straight_ref[...] = straight
    crossed_ref[...] = crossed
    arrive()

    high, low = split(recv_1[...])
    both = nn_dot(fz_hi[...], jnp.concatenate([high, low], 1))
    waves = both[:, :128] + both[:, 128:] + nn_dot(fz_lo[...], high)
    turned = turn([waves[32 * k : 32 * k + 32] for k in range(16)])
    for y in range(16):
        for c in range(2):
            send_2[pl.ds(16 * c + y, 16, stride=32), :] = turned[y][16 * c : 16 * c + 16]
    arrive, leave_2 = exchange(1, send_2, recv_2, MSG_Y, False)
    handed_first(
        live, kept, charge_ref, frac_ref, cell_ref, charge_in_order, frac_in_order, cell_in_order
    )
    arrive()

    lines = recv_2[...]
    lane = lax.broadcasted_iota(jnp.int32, (512, 128), 1)
    row = lax.broadcasted_iota(jnp.int32, (512, 128), 0)
    odd = (lane >> 3) & 1
    swapped = jnp.where(odd == 0, pltpu.roll(lines, 120, 1), pltpu.roll(lines, 8, 1))
    swapped = jnp.where((lane < 16 * (b == 0).astype(jnp.int32)), lines, swapped)
    swapped = jnp.where((row >> 4) & 1 == 0, swapped, -swapped)
    high, low = split(jnp.concatenate([lines, swapped], 1))
    waves = nn_dot(fy_hi[...], high) + nn_dot(fy_hi[...], low) + nn_dot(fy_lo[...], high)
    straight = jnp.concatenate([straight_ref[...]] * 2, 0)
    crossed = jnp.concatenate([crossed_ref[...]] * 2, 0)
    high, low = split(waves[:, :128] * straight + waves[:, 128:] * crossed)
    both = tn_dot(fy_hi[...], jnp.concatenate([high, low], 1))
    send_3[...] = (both[:, :128] + both[:, 128:] + tn_dot(fy_lo[...], high)) * (1.0 / 256)
    arrive, leave_3 = exchange(2, send_3, recv_3, MSG_Y, False)
    arrive()

    pieces = []
    for y in range(16):
        pieces.append(
            jnp.concatenate(
                [recv_3[pl.ds(16 * c + y, 16, stride=32), :] for c in range(2)], 0
            )
        )
    high, low = split(jnp.concatenate(turn(pieces), 0))
    both = tn_dot(fz_hi[...], jnp.concatenate([high, low], 1))
    send_4[...] = (both[:, :128] + both[:, 128:] + tn_dot(fz_lo[...], high)) * (1.0 / 256)
    arrive, leave_4 = exchange(3, send_4, recv_4, MSG_Z, True)
    arrive()

    turned = turn([recv_4[MSG_Z * k : MSG_Z * k + MSG_Z, :] for k in range(16)])
    lines = [jnp.concatenate([t[0:16], t[16:32]], 1) for t in turned]
    for pair in range(8):
        even, odd = turned[2 * pair][32:40], turned[2 * pair + 1][32:40]
        real = jnp.where(iota < 4, even, pltpu.roll(odd, 4, 0))
        imag = jnp.where(iota < 4, pltpu.roll(even, 4, 0), odd)
        lines.append(jnp.concatenate([real, imag], 1))
    high, low = split(jnp.concatenate(lines, 0))
    pot_ref[0:320, :] = (
        nn_dot(high, gx_hi[...]) + nn_dot(high, gx_lo[...]) + nn_dot(low, gx_hi[...])
    )

    rims = [
        pltpu.make_async_remote_copy(
            src_ref=pot_ref.at[pl.ds(source, size), :],
            dst_ref=pot_ref.at[pl.ds(target, size), :],
            send_sem=rim_sems.at[2 + 2 * k],
            recv_sem=rim_sems.at[3 + 2 * k],
            device_id=(a, before),
            device_id_type=MESH,
        )
        for k, (source, target, size) in enumerate(((0, 320, 48), (256, 368, 16)))
    ]
    for copy in rims:
        copy.start()
    leave_1()
    leave_2()
    leave_3()
    leave_4()
    for copy in rims:
        copy.wait()
    high, low = split(pot_ref[...])
    p_hi[...] = high
    p_lo[...] = low

    lent_chunks = SEND_MAX * BLOCK // CHUNK

    def compute(low, high):
        gather_atoms(
            (low, high), charge_in_order, frac_in_order, cell_in_order, forces, p_hi, p_lo
        )

    compute(0, lent_chunks)
    hand_on = pltpu.make_async_remote_copy(
        src_ref=forces.at[:, pl.ds(0, SEND_MAX * BLOCK)],
        dst_ref=guests,
        send_sem=rim_sems.at[6],
        recv_sem=rim_sems.at[7],
        device_id=(a, (b + 1) % 16),
        device_id_type=MESH,
    )
    hand_on.start()
    compute(lent_chunks, ATOMS_DEV // CHUNK)
    hand_on.wait()
    place_forces(kept, kept_before, arriving, forces, guests, out_ref)


def solve(live_blocks, send_blocks, screening, charge, fractions, cells, moduli):
    tables = []
    for table in (forward_x(), inverse_x(), forward_z(), forward_y()):
        tables += [jnp.asarray(part) for part in split_np(table)]
    message_z = pltpu.VMEM((NPEER * MSG_Z, 128), F32)
    message_y = pltpu.VMEM((NPEER * MSG_Y, 128), F32)
    return pl.pallas_call(
        solve_kernel,
        out_shape=jax.ShapeDtypeStruct((3, ATOMS_DEV), F32),
        in_specs=[pl.BlockSpec(memory_space=pltpu.SMEM)] * 3
        + [pl.BlockSpec(memory_space=pltpu.VMEM)] * (4 + len(tables)),
        out_specs=pl.BlockSpec(memory_space=pltpu.VMEM),
        scratch_shapes=[pltpu.VMEM((ROWS, GRID), F32)] * 2
        + [pltpu.VMEM((64, GRID), F32)]
        + [message_z] * 2
        + [message_y] * 4
        + [message_z] * 2
        + [pltpu.VMEM((256, 128), F32)] * 2
        + [pltpu.VMEM((320, GRID), F32)]
        + [pltpu.VMEM((ROWS, GRID), BF16)] * 2
        + [
            pltpu.VMEM((3, ATOMS_DEV), F32),
            pltpu.VMEM((3, SEND_MAX * BLOCK), F32),
            pltpu.VMEM((1, ATOMS_DEV), F32),
            pltpu.VMEM((3, ATOMS_DEV), F32),
            pltpu.VMEM((3, ATOMS_DEV), jnp.int32),
            pltpu.SemaphoreType.DMA((8,)),
            pltpu.SemaphoreType.DMA((4, NPEER)),
            pltpu.SemaphoreType.DMA((4, NPEER)),
        ],
        compiler_params=pltpu.CompilerParams(collective_id=0, has_side_effects=True),
        name="forces",
    )(live_blocks, send_blocks, screening, charge, fractions, cells, moduli, *tables)


def body(charge, fractions, cell_base, live_blocks, send_blocks, moduli, screening):
    return solve(
        live_blocks, send_blocks, screening, charge[None, :], fractions, cell_base, moduli
    )


def solution(mesh):
    return jax.shard_map(
        body,
        mesh=mesh,
        in_specs=(
            P(("gz", "gy")),
            P(None, ("gz", "gy")),
            P(None, ("gz", "gy")),
            P("gz", None),
            P("gz", None),
            P(),
            P(),
        ),
        out_specs=P(None, ("gz", "gy")),
        check_vma=False,
    )
```

```python
import functools

import jax
import jax.numpy as jnp
import numpy as np
from jax import lax
from jax.experimental import pallas as pl
from jax.experimental.pallas import tpu as pltpu
from jax.sharding import PartitionSpec as P

GRID = 256
BLOCK = 128
ATOMS_DEV = 12288
NBLK = 96
SEND_MAX = 36
NPEER = 16
CHUNK = 512
SPREAD_UNROLL = 4
GATHER_UNROLL = 6
ROWS = 384
SLOT_Z = 24
MESH = pl.DeviceIdType.MESH
BF16 = jnp.bfloat16
F32 = jnp.float32


def split_np(table):
    table = np.asarray(table, np.float32)
    high = table.astype(jnp.bfloat16)
    low = (table - high.astype(np.float32)).astype(jnp.bfloat16)
    return high, low


def kz_of(block, local):
    j = 8 * block + local // 2
    return np.where(local % 2 == 0, j, np.where(j == 0, 128, (256 - j) % 256))


def kx_order():
    stream, block, j = np.meshgrid(np.arange(2), np.arange(16), np.arange(4), indexing="ij")
    return (8 * block + 4 * stream + j).reshape(2, 64)


def forward_x():
    x = np.arange(256)[:, None]
    columns = []
    for kx in kx_order():
        angle = 2 * np.pi * ((x * kx[None, :]) % 256) / 256
        last = np.where(kx[None, :] == 0, (-1.0) ** x, -np.sin(angle))
        columns += [np.cos(angle), last]
    return np.concatenate(columns, 1)


def inverse_x():
    x = np.arange(256)[None, :]
    rows = []
    for kx in kx_order():
        angle = 2 * np.pi * ((x * kx[:, None]) % 256) / 256
        first = np.where(kx[:, None] == 0, 1.0, 2 * np.cos(angle))
        last = np.where(kx[:, None] == 0, (-1.0) ** x, -2 * np.sin(angle))
        rows += [first, last]
    return np.concatenate(rows, 0) / 256


def cos_sin(first, second):
    angle = 2 * np.pi * ((first[:, None] * second[None, :]) % 256) / 256
    return np.cos(angle), np.sin(angle)


def tables_z():
    local, block = np.meshgrid(np.arange(16), np.arange(16), indexing="ij")
    wave = kz_of(block, local).reshape(-1)
    place = np.arange(SLOT_Z)
    places = (16 * np.arange(16)[:, None] + place[None, :]).reshape(-1)
    pad = np.tile(place >= 19, 16)[None, :]
    parts = [np.where(pad, 0.0, part) for part in cos_sin(wave, places)]
    return np.concatenate(parts, 0), np.concatenate([part.T for part in parts], 0)


def table_y():
    return np.concatenate(cos_sin(np.arange(256), np.arange(256)), 0)


def split(value):
    high = value.astype(BF16)
    low = (value - high.astype(F32)).astype(BF16)
    return high, low


def spline_weights(t):
    remain = 1.0 - t
    square = t * t
    cubed = square * t
    sixth = 1.0 / 6.0
    weights = [
        remain * remain * remain * sixth,
        (3.0 * cubed - 6.0 * square + 4.0) * sixth,
        (-3.0 * cubed + 3.0 * square + 3.0 * t + 1.0) * sixth,
        cubed * sixth,
    ]
    return weights


def spline_slopes(t):
    remain = 1.0 - t
    square = t * t
    return [
        -0.5 * remain * remain,
        1.5 * square - 2.0 * t,
        -1.5 * square + t + 0.5,
        0.5 * square,
    ]


def wide(row, count):
    return jnp.broadcast_to(row, (count, row.shape[1]))


def stencil(offset, cell, weights):
    rows = offset.shape[0]
    place = offset - wide(cell, rows)
    table = jnp.zeros(offset.shape, F32)
    for k in range(3, -1, -1):
        table = jnp.where(place == k, wide(weights[k], rows), table)
    return table


def narrow_tables(cells, weights, row):
    cell = cells[row : row + 1]
    picked = [w[row : row + 1] for w in weights]
    iota = lax.broadcasted_iota(jnp.int32, (16, cell.shape[1]), 0)
    return stencil(iota, cell, picked), stencil(16 + (iota[:8] & 3), cell, picked)


def x_tables(cells, weight_sets):
    cell = cells[2:3]
    keys = [wide(((cell + m) & 255).astype(F32), 16).astype(BF16) for m in range(4)]
    sets = [[wide(w, 16).astype(BF16) for w in weights] for weights in weight_sets]
    base = lax.broadcasted_iota(jnp.int32, (16, 128), 0).astype(F32)
    results = [[] for _ in sets]
    for tile in range(16):
        place = (base + float(16 * tile)).astype(BF16)
        tables = [jnp.zeros((16, 128), BF16) for _ in sets]
        for m in range(3, -1, -1):
            hit = place == keys[m]
            tables = [jnp.where(hit, weights[m], t) for weights, t in zip(sets, tables)]
        for result, table in zip(results, tables):
            result.append(table)
    return [jnp.concatenate(result, 0) for result in results]


def high_low(rows):
    high = [w.astype(BF16).astype(F32) for w in rows]
    return high, [w - h for w, h in zip(rows, high)]


def nt_dot(a, b):
    return lax.dot_general(a, b, (((1,), (1,)), ((), ())), preferred_element_type=F32)


def nn_dot(a, b):
    return lax.dot_general(a, b, (((1,), (0,)), ((), ())), preferred_element_type=F32)


def tn_dot(a, b):
    return lax.dot_general(a, b, (((0,), (0,)), ((), ())), preferred_element_type=F32)


def pair_pattern(table, pair):
    iota = lax.broadcasted_iota(jnp.int32, (8, table.shape[1]), 0)
    return jnp.where(
        iota < 4, wide(table[2 * pair : 2 * pair + 1], 8), wide(table[2 * pair + 1 : 2 * pair + 2], 8)
    )


def plane_tables(cells, weights):
    z_main, z_halo = narrow_tables(cells, weights, 0)
    y_main, y_halo = narrow_tables(cells, weights, 1)
    pieces = [wide(y_main[y : y + 1], 16) * z_main for y in range(16)]
    pieces += [pair_pattern(y_main, pair) * z_halo for pair in range(8)]
    pieces += [wide(y_halo[y : y + 1], 16) * z_main for y in range(3)]
    pieces += [pair_pattern(y_halo, pair) * z_halo for pair in range(2)]
    return split(jnp.concatenate(pieces, 0))


def spread_atoms(live, charge_ref, frac_ref, cell_ref, tile_ref):
    n = CHUNK
    tile_ref[...] = jnp.zeros_like(tile_ref)

    def chunk(first):
        q_all = charge_ref[:, pl.ds(first, n)]
        lanes = first + lax.broadcasted_iota(jnp.int32, (1, n), 1)
        q_all = jnp.where(lanes < live, q_all, 0.0)
        weights_all = spline_weights(frac_ref[:, pl.ds(first, n)])
        cells_all = cell_ref[:, pl.ds(first, n)]
        columns = []
        for group in range(n // 128):
            lanes = slice(128 * group, 128 * group + 128)
            weights = [w[:, lanes] for w in weights_all]
            cells, q = cells_all[:, lanes], q_all[:, lanes]
            columns.append(
                tuple(x_tables(cells, high_low([w[2:3] * q for w in weights])))
                + plane_tables(cells, weights)
            )
        x_hi, x_lo, a_hi, a_lo = (jnp.concatenate(part, 1) for part in zip(*columns))
        tile_ref[...] += nt_dot(a_hi, x_hi) + nt_dot(a_hi, x_lo) + nt_dot(a_lo, x_hi)

    def step(i, carry):
        for u in range(SPREAD_UNROLL):
            chunk(pl.multiple_of((SPREAD_UNROLL * i + u) * n, n))
        return carry

    lax.fori_loop(0, ATOMS_DEV // (n * SPREAD_UNROLL), step, 0)


def gather_atoms(charge_ref, frac_ref, cell_ref, out_ref, p_hi, p_lo, when_lent_done):
    n = 256

    def piece_of(first):
        t = frac_ref[:, pl.ds(first, n)]
        cells_all = cell_ref[:, pl.ds(first, n)]
        weights_all, slopes_all = spline_weights(t), spline_slopes(t)
        columns = []
        for group in range(n // 128):
            lanes = slice(128 * group, 128 * group + 128)
            columns.append(
                x_tables(
                    cells_all[:, lanes],
                    high_low([w[2:3, lanes] for w in weights_all])
                    + high_low([w[2:3, lanes] for w in slopes_all]),
                )
            )
        w_hi, w_lo, s_hi, s_lo = (jnp.concatenate(part, 1) for part in zip(*columns))
        hi, lo = p_hi[...], p_lo[...]
        along_all = nn_dot(hi, w_hi) + nn_dot(hi, w_lo) + nn_dot(lo, w_hi)
        steep_all = nn_dot(hi, s_hi) + nn_dot(hi, s_lo) + nn_dot(lo, s_hi)
        results = []
        for group in range(n // 128):
            lanes = slice(128 * group, 128 * group + 128)
            along, steep = along_all[:, lanes], steep_all[:, lanes]
            weights = [w[:, lanes] for w in weights_all]
            slopes = [w[:, lanes] for w in slopes_all]
            cells = cells_all[:, lanes]
            zw_main, zw_halo = narrow_tables(cells, weights, 0)
            zs_main, zs_halo = narrow_tables(cells, slopes, 0)
            yw_main, yw_halo = narrow_tables(cells, weights, 1)
            ys_main, ys_halo = narrow_tables(cells, slopes, 1)
            sums = [jnp.zeros((16, 128), F32)] * 3
            for y in range(19):
                row = 16 * y if y < 16 else 320 + 16 * (y - 16)
                yw = wide(yw_main[y : y + 1] if y < 16 else yw_halo[y - 16 : y - 15], 16)
                ys = wide(ys_main[y : y + 1] if y < 16 else ys_halo[y - 16 : y - 15], 16)
                piece, slope = along[row : row + 16], steep[row : row + 16]
                sums = [sums[0] + yw * piece, sums[1] + ys * piece, sums[2] + yw * slope]
            rims = [jnp.zeros((8, 128), F32)] * 3
            for pair in range(10):
                row = 256 + 8 * pair if pair < 8 else 368 + 8 * (pair - 8)
                yw = pair_pattern(yw_main, pair) if pair < 8 else pair_pattern(yw_halo, pair - 8)
                ys = pair_pattern(ys_main, pair) if pair < 8 else pair_pattern(ys_halo, pair - 8)
                piece, slope = along[row : row + 8], steep[row : row + 8]
                rims = [rims[0] + yw * piece, rims[1] + ys * piece, rims[2] + yw * slope]
            sums = [sums[0] * zs_main, sums[1] * zw_main, sums[2] * zw_main]
            rims = [rims[0] * zs_halo, rims[1] * zw_halo, rims[2] * zw_halo]
            results.append(
                jnp.concatenate(
                    [
                        jnp.sum(f[:8] + f[8:] + r, axis=0, keepdims=True)
                        for f, r in zip(sums, rims)
                    ],
                    0,
                )
            )
        q = charge_ref[:, pl.ds(first, n)]
        out_ref[:, pl.ds(first, n)] = jnp.concatenate(results, 1) * -q

    per_step = GATHER_UNROLL * CHUNK

    def step(i, carry):
        for u in range(per_step // n):
            piece_of(pl.multiple_of(i * per_step + u * n, n))
        pl.when(i == SEND_MAX * BLOCK // per_step)(when_lent_done)
        return carry

    lax.fori_loop(0, ATOMS_DEV // per_step, step, 0)


def turn(arrays):
    arrays = list(arrays)
    rows = arrays[0].shape[0]
    group = lax.broadcasted_iota(jnp.int32, (rows, 128), 1) >> 2
    for bit in range(4):
        g = 1 << bit
        keep = (group & g) == 0
        fresh = list(arrays)
        for i in range(16):
            if i & g == 0:
                low, high = arrays[i], arrays[i | g]
                fresh[i] = jnp.where(keep, low, pltpu.roll(high, 4 * g, 1))
                fresh[i | g] = jnp.where(keep, pltpu.roll(low, 128 - 4 * g, 1), high)
        arrays = fresh
    return arrays


def tables_of_influence(moduli_ref, screening, a, b, outs):
    m = [moduli_ref[c : c + 1, :] for c in range(3)]
    lane_k = lax.broadcasted_iota(jnp.int32, (256, 256), 1)
    row_k = lax.broadcasted_iota(jnp.int32, (256, 256), 0)
    same = lane_k == row_k
    other = lane_k == ((256 - row_k) & 255)

    def column(row, mask):
        return jnp.sum(jnp.where(mask, wide(row, 256), 0.0), axis=1, keepdims=True)

    m0, m1, m2 = column(m[0], same), column(m[1], same), column(m[2], same)
    m1_back = column(m[1], other)

    lane = lax.broadcasted_iota(jnp.int32, (1, 128), 1)
    local, j = (lane >> 2) & 15, lane & 3
    step = 8 * b + (local >> 1)
    kz = jnp.where(local & 1 == 0, step, jnp.where(step == 0, 128, 256 - step))
    rows = lax.broadcasted_iota(jnp.int32, (256, 128), 0)

    def along_lanes(col, index):
        hit = rows == wide(index, 256)
        return jnp.sum(jnp.where(hit, jnp.broadcast_to(col, (256, 128)), 0.0), 0, keepdims=True)

    z0, z1 = along_lanes(m0, kz), along_lanes(m0, (256 - kz) & 255)
    def signed(k):
        return jnp.where(k < 128, k, k - 256)

    nz, ny = signed(kz), signed(rows)
    flat = ny * ny + wide(nz * nz, 256)

    def kernel_at(kx):
        nx = signed(kx)
        radius = flat + wide(nx * nx, 256)
        squared = radius.astype(F32) / float(GRID * GRID)
        safe = jnp.where(radius > 0, squared, 1.0)
        first, second = along_lanes(m2, kx), along_lanes(m2, (256 - kx) & 255)
        product = m1 * wide(z0 * first, 256) + m1_back * wide(z1 * second, 256)
        value = product * jnp.exp(-screening * squared) / safe
        return jnp.where(radius > 0, value, 0.0) * (1.0 / float(GRID * GRID))

    kx = 8 * a + j
    at_first, at_last = kernel_at(kx), kernel_at(jnp.full_like(kx, 128))
    packed = wide(kx, 256) == 0
    outs[0][...] = jnp.where(packed, 0.5 * (at_first + at_last), at_first)
    outs[1][...] = kernel_at(kx + 4)
    outs[2][...] = jnp.where(packed, 0.5 * (at_first - at_last), 0.0)


def block(ref, index):
    return ref[:, BLOCK * index : BLOCK * index + BLOCK]


def shift_left(blocks, amount, top, keep):
    bit = top
    while bit:
        take = wide((amount & bit) > 0, blocks[0].shape[0])
        count = min(len(blocks), keep + bit - 1)
        last = len(blocks) - 1
        blocks = [
            jnp.where(take, blocks[min(i + bit, last)], blocks[i]) for i in range(count)
        ]
        bit //= 2
    return blocks


def handed_first(live, kept, charge_ref, frac_ref, cell_ref, charge_out, frac_out, cell_out):
    home = NBLK - SEND_MAX
    start = jnp.minimum(jnp.full((1, BLOCK), kept, jnp.int32), home)
    count = jnp.full((1, BLOCK), live, jnp.int32)
    charges = [jnp.where(count > i, block(charge_ref, i), 0.0) for i in range(NBLK)]
    for blocks, out in (
        (charges, charge_out),
        ([block(frac_ref, i) for i in range(NBLK)], frac_out),
        ([block(cell_ref, i) for i in range(NBLK)], cell_out),
    ):
        ordered = shift_left(blocks, start, 32, SEND_MAX) + blocks[:home]
        for i, value in enumerate(ordered):
            out[:, BLOCK * i : BLOCK * i + BLOCK] = value


def place_forces(kept, kept_before, arriving, forces, guests, out_ref):
    home = NBLK - SEND_MAX
    kept = jnp.full((1, BLOCK), kept, jnp.int32)
    kept_before = jnp.full((1, BLOCK), kept_before, jnp.int32)
    end = kept + arriving
    skip = kept_before - jnp.minimum(kept_before, home)
    arrived = shift_left([block(guests, i) for i in range(SEND_MAX)], skip, 32, SEND_MAX)
    placed = arrived + [jnp.zeros((3, BLOCK), F32)] * (NBLK - SEND_MAX)
    bit = 64
    while bit:
        take = wide((kept & bit) > 0, 3)
        placed = [
            jnp.where(take, placed[i - bit] if i >= bit else 0.0, placed[i]) for i in range(NBLK)
        ]
        bit //= 2
    for slot in range(NBLK):
        own = block(forces, SEND_MAX + slot if slot < home else slot - home)
        guest = jnp.where(wide(end > slot, 3), placed[slot], 0.0)
        out_ref[:, BLOCK * slot : BLOCK * slot + BLOCK] = jnp.where(wide(kept > slot, 3), own, guest)


def offsets_z():
    return [(dz, dy) for dz in (4, 3, -3, 2, -2, 1, -1, 0) for dy in (1, 0) if (dz, dy) != (0, 0)]


def offsets_y():
    moves = [(dx, dy, dc) for dx in (2, 1, -1, 0) for dy in (1, 0) for dc in (1, 0)]
    moves.remove((0, 0, 0))
    return sorted(moves, key=lambda m: -(abs(m[0]) + 2 * m[1]))


def solve_kernel(
    live_ref,
    send_ref,
    screening_ref,
    charge_ref,
    frac_ref,
    cell_ref,
    moduli_ref,
    fx_far,
    gx_far,
    fz_far,
    gz_far,
    fy_far,
    out_ref,
    fx,
    gx,
    fz,
    gz,
    fy,
    table_sems,
    tile_ref,
    pot_ref,
    rim_in,
    send_10,
    recv_10,
    send_11,
    recv_11,
    send_2,
    recv_2,
    send_3,
    recv_3,
    send_40,
    recv_40,
    send_41,
    recv_41,
    straight_0,
    straight_1,
    crossed_0,
    p_hi,
    p_lo,
    forces,
    guests,
    charge_in_order,
    frac_in_order,
    cell_in_order,
    held_1,
    held_4,
    rim_sems,
    relay_sems,
    send_sems,
    recv_sems,
):
    a, b = lax.axis_index("gz"), lax.axis_index("gy")
    barrier = pltpu.get_barrier_semaphore()
    peers_z = [
        ((a // 2 + dz + 8) % 8) * 2 + (a + dy) % 2 for dz, dy in offsets_z()
    ]
    peers_y = [
        ((b // 4 + dx + 4) % 4) * 4 + ((b // 2 + dy) % 2) * 2 + (b + dc) % 2
        for dx, dy, dc in offsets_y()
    ]
    for peer in peers_z:
        pl.semaphore_signal(barrier, inc=1, device_id=(peer, b), device_id_type=MESH)
    for peer in peers_y:
        pl.semaphore_signal(barrier, inc=1, device_id=(a, peer), device_id_type=MESH)

    loads = [
        pltpu.make_async_copy(far, near, table_sems.at[k])
        for k, (far, near) in enumerate(
            ((fx_far, fx), (fz_far, fz), (fy_far, fy), (gz_far, gz), (gx_far, gx))
        )
    ]
    for load in loads:
        load.start()

    before = (b + 15) % 16
    live = live_ref[0, b]
    kept = live - send_ref[0, b]
    kept_before = live_ref[0, before] - send_ref[0, before]
    arriving = send_ref[0, before]
    spread_atoms(live * BLOCK, charge_ref, frac_ref, cell_ref, tile_ref)
    for load in loads:
        load.wait()
    pl.semaphore_wait(barrier, 2 * (NPEER - 1))

    leaving = []

    def exchange(stage, src, dst, size, over_z, relay=None):
        me = a if over_z else b
        peers = peers_z if over_z else peers_y
        whole = pl.ds(0, (NPEER - 1) * size)

        def rows_of(index):
            return pl.ds(pl.multiple_of(index * size, 8), size)

        def copy(source, target, peer, send_sem, recv_sem):
            return pltpu.make_async_remote_copy(
                src_ref=source,
                dst_ref=target,
                send_sem=send_sem,
                recv_sem=recv_sem,
                device_id=(peer, b) if over_z else (a, peer),
                device_id_type=MESH,
            )

        send_sem, recv_sem = send_sems.at[stage], recv_sems.at[stage]
        passing = []
        if relay is not None:
            buffer, sems = relay
            step = (a // 2 + 6) % 8 * 2
            origin = (a // 2 + 2) % 8 * 2 + a % 2
            for k in range(2):
                held = buffer.at[pl.ds(k * size, size), :]
                copy(
                    src.at[rows_of(peers[k]), :], held, step + a % 2, send_sem, relay_sems.at[sems]
                ).start()
                passing.append(
                    copy(
                        held,
                        dst.at[rows_of(origin), :],
                        step + (a + 1 - k) % 2,
                        relay_sems.at[sems + 1],
                        recv_sem,
                    )
                )
            peers = peers[2:]
        for peer in peers:
            copy(src.at[rows_of(peer), :], dst.at[rows_of(me), :], peer, send_sem, recv_sem).start()
        dst[rows_of(me), :] = src[rows_of(me), :]
        every = copy(src.at[whole, :], dst.at[whole, :], peers[0], send_sem, recv_sem)
        leaving.append(every.wait_send)
        if relay is not None:
            both = pl.ds(0, 2 * size)
            held = copy(
                buffer.at[both, :],
                buffer.at[both, :],
                peers[0],
                relay_sems.at[sems + 1],
                relay_sems.at[sems],
            )
            leaving.append(held.wait_send)

            def forward():
                held.wait_recv()
                for message in passing:
                    message.start()

            return every.wait_recv, forward
        return every.wait_recv

    rim = pltpu.make_async_remote_copy(
        src_ref=tile_ref.at[pl.ds(320, 64), :],
        dst_ref=rim_in,
        send_sem=rim_sems.at[0],
        recv_sem=rim_sems.at[1],
        device_id=(a, (b + 1) % 16),
        device_id_type=MESH,
    )
    rim.start()

    def transform_x(value):
        high, low = split(value)
        return nn_dot(high, fx[0]) + nn_dot(high, fx[1]) + nn_dot(low, fx[0])

    spectrum = transform_x(tile_ref[0:320, :])
    rim.wait()
    extra = transform_x(rim_in[...])
    spectrum = jnp.concatenate(
        [
            spectrum[0:48] + extra[0:48],
            spectrum[48:256],
            spectrum[256:272] + extra[48:64],
            spectrum[272:320],
        ],
        0,
    )
    iota = lax.broadcasted_iota(jnp.int32, (8, 128), 0)
    pieces = []
    for y in range(16):
        row = 256 + 8 * (y // 2)
        first, second = spectrum[row : row + 8, :128], spectrum[row : row + 8, 128:]
        if y % 2 == 0:
            halo = jnp.where(iota < 4, first, pltpu.roll(second, 4, 0))
        else:
            halo = jnp.where(iota < 4, pltpu.roll(first, 4, 0), second)
        pieces.append(jnp.concatenate([spectrum[16 * y : 16 * y + 16, :128], halo], 0))
    for peer, piece in enumerate(turn(pieces)):
        send_10[24 * peer : 24 * peer + 24, :] = piece
    arrive_10 = exchange(0, send_10, recv_10, 24, True)
    for peer, piece in enumerate(turn([spectrum[16 * y : 16 * y + 16, 128:] for y in range(16)])):
        send_11[16 * peer : 16 * peer + 16, :] = piece
    arrive_11, forward = exchange(1, send_11, recv_11, 16, True, (held_1, 0))
    tables_of_influence(
        moduli_ref, screening_ref[0], a, b, (straight_0, straight_1, crossed_0)
    )
    forward()

    half = lax.broadcasted_iota(jnp.int32, (1, 128), 1) < 64
    forward_sign = jnp.where(half, 1.0, -1.0)

    def product(table, value):
        high, low = split(value)
        width = value.shape[1]
        both = nn_dot(table[0], jnp.concatenate([high, low], 1))
        return both[:, :width] + both[:, width:] + nn_dot(table[1], high)

    def joined(both, sign):
        rows = both.shape[0] // 2
        return both[:rows] + wide(sign, rows) * pltpu.roll(both[rows:], 64, 1)

    def stage_z(stream):
        if stream == 0:
            lines = recv_10[...]
        else:
            lines = []
            for k in range(16):
                lines += [
                    recv_11[16 * k : 16 * k + 16, :],
                    pltpu.roll(recv_10[24 * k + 16 : 24 * k + 24, :], 4, 0),
                ]
            lines = jnp.concatenate(lines, 0)
        waves = joined(product(fz, lines), forward_sign)
        turned = turn([waves[16 * k : 16 * k + 16] for k in range(16)])
        for y in range(16):
            send_2[pl.ds(256 * stream + y, 16, stride=16), :] = turned[y]
        rows = pl.ds(256 * stream, 256)
        return exchange(2 + stream, send_2.at[rows, :], recv_2.at[rows, :], 16, False)

    def stage_y(stream):
        lines = recv_2[256 * stream : 256 * stream + 256, :]
        if stream == 0:
            lane = lax.broadcasted_iota(jnp.int32, (256, 128), 1)
            odd = (lane >> 2) & 1
            swapped = jnp.where(odd == 0, pltpu.roll(lines, 124, 1), pltpu.roll(lines, 4, 1))
            own_pair = wide(((lax.broadcasted_iota(jnp.int32, (1, 128), 1) & 63) >> 3) + b, 256) == 0
            swapped = jnp.where(own_pair, lines, swapped)
            both = product(fy, jnp.concatenate([lines, swapped * wide(forward_sign, 256)], 1))
            waves = joined(both[:, :128], forward_sign) * straight_0[...]
            waves = waves + joined(both[:, 128:], forward_sign) * crossed_0[...]
        else:
            waves = joined(product(fy, lines), forward_sign) * straight_1[...]
        rows = pl.ds(256 * stream, 256)
        send_3[rows, :] = joined(product(fy, waves), -forward_sign)
        return exchange(4 + stream, send_3.at[rows, :], recv_3.at[rows, :], 16, False)

    def stage_z_back(stream):
        pieces = [recv_3[pl.ds(256 * stream + y, 16, stride=16), :] for y in range(16)]
        lines = jnp.concatenate(turn(pieces), 0)
        return joined(product(gz, lines), -forward_sign)

    arrive_10()
    arrive_20 = stage_z(0)
    arrive_11()
    arrive_21 = stage_z(1)
    arrive_20()
    arrive_30 = stage_y(0)
    arrive_21()
    arrive_31 = stage_y(1)
    arrive_30()
    back = stage_z_back(0)
    for k in range(16):
        send_40[16 * k : 16 * k + 16, :] = back[24 * k : 24 * k + 16]
        send_41[24 * k + 16 : 24 * k + 24, :] = back[24 * k + 16 : 24 * k + 24]
    arrive_40 = exchange(6, send_40, recv_40, 16, True)
    arrive_31()
    back = stage_z_back(1)
    for k in range(16):
        send_41[24 * k : 24 * k + 16, :] = back[24 * k : 24 * k + 16]
        send_41[24 * k + 16 : 24 * k + 24, :] += pltpu.roll(back[24 * k + 16 : 24 * k + 24], 4, 0)
    arrive_41, forward = exchange(7, send_41, recv_41, 24, True, (held_4, 2))
    handed_first(
        live, kept, charge_ref, frac_ref, cell_ref, charge_in_order, frac_in_order, cell_in_order
    )
    forward()
    arrive_40()
    turned_0 = turn([recv_40[16 * k : 16 * k + 16, :] for k in range(16)])
    arrive_41()
    turned_1 = turn([recv_41[24 * k : 24 * k + 24, :] for k in range(16)])

    lines = [jnp.concatenate([first, second[:16]], 1) for first, second in zip(turned_0, turned_1)]
    rims = []
    for pair in range(8):
        even, odd = turned_1[2 * pair][16:24], turned_1[2 * pair + 1][16:24]
        first = jnp.where(iota < 4, even, pltpu.roll(odd, 4, 0))
        second = jnp.where(iota < 4, pltpu.roll(even, 4, 0), odd)
        rims.append(jnp.concatenate([first, second], 1))

    def back_x(value):
        high, low = split(value)
        return nn_dot(high, gx[0]) + nn_dot(high, gx[1]) + nn_dot(low, gx[0])

    value = back_x(jnp.concatenate(lines[:3] + rims[:2], 0))
    pot_ref[0:48, :] = value[0:48]
    pot_ref[256:272, :] = value[48:64]
    copies = [
        pltpu.make_async_remote_copy(
            src_ref=pot_ref.at[pl.ds(source, size), :],
            dst_ref=pot_ref.at[pl.ds(target, size), :],
            send_sem=rim_sems.at[2 + 2 * k],
            recv_sem=rim_sems.at[3 + 2 * k],
            device_id=(a, before),
            device_id_type=MESH,
        )
        for k, (source, target, size) in enumerate(((0, 320, 48), (256, 368, 16)))
    ]
    for copy in copies:
        copy.start()
    value = back_x(jnp.concatenate(lines[3:] + rims[2:], 0))
    pot_ref[48:256, :] = value[:208]
    pot_ref[272:320, :] = value[208:]
    for leave in leaving:
        leave()
    for copy in copies:
        copy.wait()
    high, low = split(pot_ref[...])
    p_hi[...] = high
    p_lo[...] = low

    hand_on = pltpu.make_async_remote_copy(
        src_ref=forces.at[:, pl.ds(0, SEND_MAX * BLOCK)],
        dst_ref=guests,
        send_sem=rim_sems.at[6],
        recv_sem=rim_sems.at[7],
        device_id=(a, (b + 1) % 16),
        device_id_type=MESH,
    )
    gather_atoms(
        charge_in_order, frac_in_order, cell_in_order, forces, p_hi, p_lo, hand_on.start
    )
    hand_on.wait()
    place_forces(kept, kept_before, arriving, forces, guests, out_ref)


def solve(live_blocks, send_blocks, screening, charge, fractions, cells, moduli):
    tables = []
    for table in (forward_x(), inverse_x(), *tables_z(), table_y()):
        tables.append(jnp.asarray(np.stack(split_np(table))))
    short, tall = pltpu.VMEM((256, 128), F32), pltpu.VMEM((384, 128), F32)
    both = pltpu.VMEM((512, 128), F32)
    return pl.pallas_call(
        solve_kernel,
        out_shape=jax.ShapeDtypeStruct((3, ATOMS_DEV), F32),
        in_specs=[pl.BlockSpec(memory_space=pltpu.SMEM)] * 3
        + [pl.BlockSpec(memory_space=pltpu.VMEM)] * 4
        + [pl.BlockSpec(memory_space=pltpu.HBM)] * len(tables),
        out_specs=pl.BlockSpec(memory_space=pltpu.VMEM),
        scratch_shapes=[pltpu.VMEM(table.shape, BF16) for table in tables]
        + [pltpu.SemaphoreType.DMA((len(tables),))]
        + [pltpu.VMEM((ROWS, GRID), F32)] * 2
        + [pltpu.VMEM((64, GRID), F32)]
        + [tall] * 2
        + [short] * 2
        + [both] * 4
        + [short] * 2
        + [tall] * 2
        + [short] * 3
        + [pltpu.VMEM((ROWS, GRID), BF16)] * 2
        + [
            pltpu.VMEM((3, ATOMS_DEV), F32),
            pltpu.VMEM((3, SEND_MAX * BLOCK), F32),
            pltpu.VMEM((1, ATOMS_DEV), F32),
            pltpu.VMEM((3, ATOMS_DEV), F32),
            pltpu.VMEM((3, ATOMS_DEV), jnp.int32),
            pltpu.VMEM((32, 128), F32),
            pltpu.VMEM((48, 128), F32),
            pltpu.SemaphoreType.DMA((8,)),
            pltpu.SemaphoreType.DMA((4,)),
            pltpu.SemaphoreType.DMA((8,)),
            pltpu.SemaphoreType.DMA((8,)),
        ],
        compiler_params=pltpu.CompilerParams(collective_id=0, has_side_effects=True),
        name="forces",
    )(live_blocks, send_blocks, screening, charge, fractions, cells, moduli, *tables)


def body(charge, fractions, cell_base, live_blocks, send_blocks, moduli, screening):
    return solve(
        live_blocks, send_blocks, screening, charge[None, :], fractions, cell_base, moduli
    )


def solution(mesh):
    return jax.shard_map(
        body,
        mesh=mesh,
        in_specs=(
            P(("gz", "gy")),
            P(None, ("gz", "gy")),
            P(None, ("gz", "gy")),
            P("gz", None),
            P("gz", None),
            P(),
            P(),
        ),
        out_specs=P(None, ("gz", "gy")),
        check_vma=False,
    )
```

```python
import functools

import jax
import jax.numpy as jnp
import numpy as np
from jax import lax
from jax.experimental import pallas as pl
from jax.experimental.pallas import tpu as pltpu
from jax.sharding import PartitionSpec as P

GRID = 256
BLOCK = 128
ATOMS_DEV = 12288
NBLK = 96
SEND_MAX = 36
NPEER = 16
CHUNK = 512
SPREAD_UNROLL = 4
GATHER_UNROLL = 4
EARLY = 8
CORE = 256
ROWS = 384
MESH = pl.DeviceIdType.MESH
BF16 = jnp.bfloat16
F32 = jnp.float32


def split_np(table):
    table = np.asarray(table, np.float32)
    high = table.astype(jnp.bfloat16)
    low = (table - high.astype(np.float32)).astype(jnp.bfloat16)
    return high, low


def kz_of(block, local):
    j = 8 * block + local // 2
    return np.where(local % 2 == 0, j, np.where(j == 0, 128, (256 - j) % 256))


def kx_order():
    stream, block, j = np.meshgrid(np.arange(2), np.arange(16), np.arange(4), indexing="ij")
    return (8 * block + 4 * stream + j).reshape(2, 64)


def forward_x():
    x = np.arange(256)[:, None]
    columns = []
    for kx in kx_order():
        angle = 2 * np.pi * ((x * kx[None, :]) % 256) / 256
        last = np.where(kx[None, :] == 0, (-1.0) ** x, -np.sin(angle))
        columns += [np.cos(angle), last]
    return np.concatenate(columns, 1)


def inverse_x():
    x = np.arange(256)[None, :]
    rows = []
    for kx in kx_order():
        angle = 2 * np.pi * ((x * kx[:, None]) % 256) / 256
        first = np.where(kx[:, None] == 0, 1.0, 2 * np.cos(angle))
        last = np.where(kx[:, None] == 0, (-1.0) ** x, -2 * np.sin(angle))
        rows += [first, last]
    return np.concatenate(rows, 0) / 256


def cos_sin(first, second):
    angle = 2 * np.pi * ((first[:, None] * second[None, :]) % 256) / 256
    return np.cos(angle), np.sin(angle)


def tables_z():
    local, block = np.meshgrid(np.arange(16), np.arange(16), indexing="ij")
    parts = cos_sin(kz_of(block, local).reshape(-1), np.arange(256))
    return np.concatenate(parts, 0), np.concatenate([part.T for part in parts], 0)


def table_y():
    return np.concatenate(cos_sin(np.arange(256), np.arange(256)), 0)


def split(value):
    high = value.astype(BF16)
    low = (value - high.astype(F32)).astype(BF16)
    return high, low


def spline_weights(t):
    remain = 1.0 - t
    square = t * t
    cubed = square * t
    sixth = 1.0 / 6.0
    weights = [
        remain * remain * remain * sixth,
        (3.0 * cubed - 6.0 * square + 4.0) * sixth,
        (-3.0 * cubed + 3.0 * square + 3.0 * t + 1.0) * sixth,
        cubed * sixth,
    ]
    return weights


def spline_slopes(t):
    remain = 1.0 - t
    square = t * t
    return [
        -0.5 * remain * remain,
        1.5 * square - 2.0 * t,
        -1.5 * square + t + 0.5,
        0.5 * square,
    ]


def wide(row, count):
    return jnp.broadcast_to(row, (count, row.shape[1]))


def stencil(offset, cell, weights):
    rows = offset.shape[0]
    place = offset - wide(cell, rows)
    table = jnp.zeros(offset.shape, F32)
    for k in range(3, -1, -1):
        table = jnp.where(place == k, wide(weights[k], rows), table)
    return table


def narrow_tables(cells, weights, row):
    cell = cells[row : row + 1]
    picked = [w[row : row + 1] for w in weights]
    iota = lax.broadcasted_iota(jnp.int32, (16, cell.shape[1]), 0)
    return stencil(iota, cell, picked), stencil(16 + (iota[:8] & 3), cell, picked)


def x_tables(cells, weight_sets):
    cell = cells[2:3]
    keys = [wide(((cell + m) & 255).astype(F32), 16).astype(BF16) for m in range(4)]
    sets = [[wide(w, 16).astype(BF16) for w in weights] for weights in weight_sets]
    base = lax.broadcasted_iota(jnp.int32, (16, 128), 0).astype(F32)
    results = [[] for _ in sets]
    for tile in range(16):
        place = (base + float(16 * tile)).astype(BF16)
        tables = [jnp.zeros((16, 128), BF16) for _ in sets]
        for m in range(3, -1, -1):
            hit = place == keys[m]
            tables = [jnp.where(hit, weights[m], t) for weights, t in zip(sets, tables)]
        for result, table in zip(results, tables):
            result.append(table)
    return [jnp.concatenate(result, 0) for result in results]


def high_low(rows):
    high = [w.astype(BF16).astype(F32) for w in rows]
    return high, [w - h for w, h in zip(rows, high)]


def nt_dot(a, b):
    return lax.dot_general(a, b, (((1,), (1,)), ((), ())), preferred_element_type=F32)


def nn_dot(a, b):
    return lax.dot_general(a, b, (((1,), (0,)), ((), ())), preferred_element_type=F32)


def tn_dot(a, b):
    return lax.dot_general(a, b, (((0,), (0,)), ((), ())), preferred_element_type=F32)


def pair_pattern(table, pair):
    iota = lax.broadcasted_iota(jnp.int32, (8, table.shape[1]), 0)
    return jnp.where(
        iota < 4, wide(table[2 * pair : 2 * pair + 1], 8), wide(table[2 * pair + 1 : 2 * pair + 2], 8)
    )


def plane_tables(cells, weights):
    z_main, z_halo = narrow_tables(cells, weights, 0)
    y_main, y_halo = narrow_tables(cells, weights, 1)
    pieces = [wide(y_main[y : y + 1], 16) * z_main for y in range(16)]
    pieces += [pair_pattern(y_main, pair) * z_halo for pair in range(8)]
    pieces += [wide(y_halo[y : y + 1], 16) * z_main for y in range(3)]
    pieces += [pair_pattern(y_halo, pair) * z_halo for pair in range(2)]
    return split(jnp.concatenate(pieces, 0))


def spread_atoms(live, charge_ref, frac_ref, cell_ref, tile_ref):
    n = CHUNK
    tile_ref[...] = jnp.zeros_like(tile_ref)

    def chunk(first):
        q_all = charge_ref[:, pl.ds(first, n)]
        lanes = first + lax.broadcasted_iota(jnp.int32, (1, n), 1)
        q_all = jnp.where(lanes < live, q_all, 0.0)
        weights_all = spline_weights(frac_ref[:, pl.ds(first, n)])
        cells_all = cell_ref[:, pl.ds(first, n)]
        columns = []
        for group in range(n // 128):
            lanes = slice(128 * group, 128 * group + 128)
            weights = [w[:, lanes] for w in weights_all]
            cells, q = cells_all[:, lanes], q_all[:, lanes]
            columns.append(
                tuple(x_tables(cells, high_low([w[2:3] * q for w in weights])))
                + plane_tables(cells, weights)
            )
        x_hi, x_lo, a_hi, a_lo = (jnp.concatenate(part, 1) for part in zip(*columns))
        tile_ref[...] += nt_dot(a_hi, x_hi) + nt_dot(a_hi, x_lo) + nt_dot(a_lo, x_hi)

    def step(i, carry):
        for u in range(SPREAD_UNROLL):
            chunk(pl.multiple_of((SPREAD_UNROLL * i + u) * n, n))
        return carry

    lax.fori_loop(0, ATOMS_DEV // (n * SPREAD_UNROLL), step, 0)


def gather_atoms(
    chunks, own, rim, charge_ref, frac_ref, cell_ref, out_ref, p_hi, p_lo, after_first=None
):
    base = 0 if own else CORE
    rows = slice(base, ROWS if rim else CORE)
    n = 256

    def piece_of(first):
        t = frac_ref[:, pl.ds(first, n)]
        cells_all = cell_ref[:, pl.ds(first, n)]
        weights_all, slopes_all = spline_weights(t), spline_slopes(t)
        columns = []
        for group in range(n // 128):
            lanes = slice(128 * group, 128 * group + 128)
            columns.append(
                x_tables(
                    cells_all[:, lanes],
                    high_low([w[2:3, lanes] for w in weights_all])
                    + high_low([w[2:3, lanes] for w in slopes_all]),
                )
            )
        w_hi, w_lo, s_hi, s_lo = (jnp.concatenate(part, 1) for part in zip(*columns))
        hi, lo = p_hi[rows, :], p_lo[rows, :]
        along_all = nn_dot(hi, w_hi) + nn_dot(hi, w_lo) + nn_dot(lo, w_hi)
        steep_all = nn_dot(hi, s_hi) + nn_dot(hi, s_lo) + nn_dot(lo, s_hi)
        results = []
        for group in range(n // 128):
            lanes = slice(128 * group, 128 * group + 128)
            along, steep = along_all[:, lanes], steep_all[:, lanes]
            weights = [w[:, lanes] for w in weights_all]
            slopes = [w[:, lanes] for w in slopes_all]
            cells = cells_all[:, lanes]
            zw_main, zw_halo = narrow_tables(cells, weights, 0)
            zs_main, zs_halo = narrow_tables(cells, slopes, 0)
            yw_main, yw_halo = narrow_tables(cells, weights, 1)
            ys_main, ys_halo = narrow_tables(cells, slopes, 1)
            sums = [jnp.zeros((16, 128), F32)] * 3
            for y in range(0 if own else 16, 19 if rim else 16):
                row = 16 * y if y < 16 else 320 + 16 * (y - 16) - base
                yw = wide(yw_main[y : y + 1] if y < 16 else yw_halo[y - 16 : y - 15], 16)
                ys = wide(ys_main[y : y + 1] if y < 16 else ys_halo[y - 16 : y - 15], 16)
                piece, slope = along[row : row + 16], steep[row : row + 16]
                sums = [sums[0] + yw * piece, sums[1] + ys * piece, sums[2] + yw * slope]
            rims = [jnp.zeros((8, 128), F32)] * 3
            for pair in range(10 if rim else 0):
                row = (256 + 8 * pair if pair < 8 else 368 + 8 * (pair - 8)) - base
                yw = pair_pattern(yw_main, pair) if pair < 8 else pair_pattern(yw_halo, pair - 8)
                ys = pair_pattern(ys_main, pair) if pair < 8 else pair_pattern(ys_halo, pair - 8)
                piece, slope = along[row : row + 8], steep[row : row + 8]
                rims = [rims[0] + yw * piece, rims[1] + ys * piece, rims[2] + yw * slope]
            sums = [sums[0] * zs_main, sums[1] * zw_main, sums[2] * zw_main]
            rims = [rims[0] * zs_halo, rims[1] * zw_halo, rims[2] * zw_halo]
            results.append(
                jnp.concatenate(
                    [
                        jnp.sum(f[:8] + f[8:] + r, axis=0, keepdims=True)
                        for f, r in zip(sums, rims)
                    ],
                    0,
                )
            )
        q = charge_ref[:, pl.ds(first, n)]
        result = jnp.concatenate(results, 1) * -q
        if not own:
            result = result + out_ref[:, pl.ds(first, n)]
        out_ref[:, pl.ds(first, n)] = result

    low, high = chunks
    per_step = GATHER_UNROLL * CHUNK

    def step(i, carry):
        for u in range(per_step // n):
            piece_of(pl.multiple_of(low * CHUNK + i * per_step + u * n, n))
        if after_first is not None:
            pl.when(i == 0)(after_first)
        return carry

    lax.fori_loop(0, (high - low) // GATHER_UNROLL, step, 0)


def turn(arrays):
    arrays = list(arrays)
    rows = arrays[0].shape[0]
    group = lax.broadcasted_iota(jnp.int32, (rows, 128), 1) >> 2
    for bit in range(4):
        g = 1 << bit
        keep = (group & g) == 0
        fresh = list(arrays)
        for i in range(16):
            if i & g == 0:
                low, high = arrays[i], arrays[i | g]
                fresh[i] = jnp.where(keep, low, pltpu.roll(high, 4 * g, 1))
                fresh[i | g] = jnp.where(keep, pltpu.roll(low, 128 - 4 * g, 1), high)
        arrays = fresh
    return arrays


def tables_of_influence(moduli_ref, screening, a, b, outs):
    m = [moduli_ref[c : c + 1, :] for c in range(3)]
    lane_k = lax.broadcasted_iota(jnp.int32, (256, 256), 1)
    row_k = lax.broadcasted_iota(jnp.int32, (256, 256), 0)
    same = lane_k == row_k
    other = lane_k == ((256 - row_k) & 255)

    def column(row, mask):
        return jnp.sum(jnp.where(mask, wide(row, 256), 0.0), axis=1, keepdims=True)

    m0, m1, m2 = column(m[0], same), column(m[1], same), column(m[2], same)
    m1_back = column(m[1], other)

    lane = lax.broadcasted_iota(jnp.int32, (1, 128), 1)
    local, j = (lane >> 2) & 15, lane & 3
    step = 8 * b + (local >> 1)
    kz = jnp.where(local & 1 == 0, step, jnp.where(step == 0, 128, 256 - step))
    rows = lax.broadcasted_iota(jnp.int32, (256, 128), 0)

    def along_lanes(col, index):
        hit = rows == wide(index, 256)
        return jnp.sum(jnp.where(hit, jnp.broadcast_to(col, (256, 128)), 0.0), 0, keepdims=True)

    z0, z1 = along_lanes(m0, kz), along_lanes(m0, (256 - kz) & 255)
    def signed(k):
        return jnp.where(k < 128, k, k - 256)

    nz, ny = signed(kz), signed(rows)
    flat = ny * ny + wide(nz * nz, 256)

    def kernel_at(kx):
        nx = signed(kx)
        radius = flat + wide(nx * nx, 256)
        squared = radius.astype(F32) / float(GRID * GRID)
        safe = jnp.where(radius > 0, squared, 1.0)
        first, second = along_lanes(m2, kx), along_lanes(m2, (256 - kx) & 255)
        product = m1 * wide(z0 * first, 256) + m1_back * wide(z1 * second, 256)
        value = product * jnp.exp(-screening * squared) / safe
        return jnp.where(radius > 0, value, 0.0) * (1.0 / float(GRID * GRID))

    kx = 8 * a + j
    at_first, at_last = kernel_at(kx), kernel_at(jnp.full_like(kx, 128))
    packed = wide(kx, 256) == 0
    outs[0][...] = jnp.where(packed, 0.5 * (at_first + at_last), at_first)
    outs[1][...] = kernel_at(kx + 4)
    outs[2][...] = jnp.where(packed, 0.5 * (at_first - at_last), 0.0)


def block(ref, index):
    return ref[:, BLOCK * index : BLOCK * index + BLOCK]


def shift_left(blocks, amount, top, keep):
    bit = top
    while bit:
        take = wide((amount & bit) > 0, blocks[0].shape[0])
        count = min(len(blocks), keep + bit - 1)
        last = len(blocks) - 1
        blocks = [
            jnp.where(take, blocks[min(i + bit, last)], blocks[i]) for i in range(count)
        ]
        bit //= 2
    return blocks


def handed_first(live, kept, charge_ref, frac_ref, cell_ref, charge_out, frac_out, cell_out):
    home = NBLK - SEND_MAX
    start = jnp.minimum(jnp.full((1, BLOCK), kept, jnp.int32), home)
    count = jnp.full((1, BLOCK), live, jnp.int32)
    charges = [jnp.where(count > i, block(charge_ref, i), 0.0) for i in range(NBLK)]
    for blocks, out in (
        (charges, charge_out),
        ([block(frac_ref, i) for i in range(NBLK)], frac_out),
        ([block(cell_ref, i) for i in range(NBLK)], cell_out),
    ):
        ordered = shift_left(blocks, start, 32, SEND_MAX) + blocks[:home]
        for i, value in enumerate(ordered):
            out[:, BLOCK * i : BLOCK * i + BLOCK] = value


def place_forces(kept, kept_before, arriving, forces, guests, out_ref):
    home = NBLK - SEND_MAX
    kept = jnp.full((1, BLOCK), kept, jnp.int32)
    kept_before = jnp.full((1, BLOCK), kept_before, jnp.int32)
    end = kept + arriving
    skip = kept_before - jnp.minimum(kept_before, home)
    arrived = shift_left([block(guests, i) for i in range(SEND_MAX)], skip, 32, SEND_MAX)
    placed = arrived + [jnp.zeros((3, BLOCK), F32)] * (NBLK - SEND_MAX)
    bit = 64
    while bit:
        take = wide((kept & bit) > 0, 3)
        placed = [
            jnp.where(take, placed[i - bit] if i >= bit else 0.0, placed[i]) for i in range(NBLK)
        ]
        bit //= 2
    for slot in range(NBLK):
        own = block(forces, SEND_MAX + slot if slot < home else slot - home)
        guest = jnp.where(wide(end > slot, 3), placed[slot], 0.0)
        out_ref[:, BLOCK * slot : BLOCK * slot + BLOCK] = jnp.where(wide(kept > slot, 3), own, guest)


def offsets_z():
    return [(dz, dy) for dz in (4, 3, -3, 2, -2, 1, -1, 0) for dy in (1, 0) if (dz, dy) != (0, 0)]


def offsets_y():
    moves = [(dx, dy, dc) for dx in (2, 1, -1, 0) for dy in (1, 0) for dc in (1, 0)]
    moves.remove((0, 0, 0))
    return sorted(moves, key=lambda m: -(abs(m[0]) + 2 * m[1]))


def solve_kernel(
    live_ref,
    send_ref,
    screening_ref,
    charge_ref,
    frac_ref,
    cell_ref,
    moduli_ref,
    fx_far,
    gx_far,
    fz_far,
    gz_far,
    fy_far,
    out_ref,
    fx,
    gx,
    fz,
    gz,
    fy,
    table_sems,
    tile_ref,
    pot_ref,
    rim_in,
    planes_out,
    send_1,
    recv_1,
    send_2,
    recv_2,
    send_3,
    recv_3,
    send_4,
    recv_4,
    straight_0,
    straight_1,
    crossed_0,
    p_hi,
    p_lo,
    forces,
    guests,
    charge_in_order,
    frac_in_order,
    cell_in_order,
    held_1,
    held_4,
    rim_sems,
    relay_sems,
    send_sems,
    recv_sems,
):
    a, b = lax.axis_index("gz"), lax.axis_index("gy")
    barrier = pltpu.get_barrier_semaphore()
    peers_z = [
        ((a // 2 + dz + 8) % 8) * 2 + (a + dy) % 2 for dz, dy in offsets_z()
    ]
    peers_y = [
        ((b // 4 + dx + 4) % 4) * 4 + ((b // 2 + dy) % 2) * 2 + (b + dc) % 2
        for dx, dy, dc in offsets_y()
    ]
    for peer in peers_z:
        pl.semaphore_signal(barrier, inc=1, device_id=(peer, b), device_id_type=MESH)
    for peer in peers_y:
        pl.semaphore_signal(barrier, inc=1, device_id=(a, peer), device_id_type=MESH)

    loads = [
        pltpu.make_async_copy(far, near, table_sems.at[k])
        for k, (far, near) in enumerate(
            ((fx_far, fx), (fz_far, fz), (fy_far, fy), (gz_far, gz), (gx_far, gx))
        )
    ]
    for load in loads:
        load.start()

    before, after = (b + 15) % 16, (b + 1) % 16
    before_z, after_z = (a + 15) % 16, (a + 1) % 16
    for peer in ((before_z, before), (after_z, after)):
        pl.semaphore_signal(barrier, inc=1, device_id=peer, device_id_type=MESH)
    live = live_ref[0, b]
    kept = live - send_ref[0, b]
    kept_before = live_ref[0, before] - send_ref[0, before]
    arriving = send_ref[0, before]
    spread_atoms(live * BLOCK, charge_ref, frac_ref, cell_ref, tile_ref)
    for load in loads:
        load.wait()
    pl.semaphore_wait(barrier, 2 * NPEER)

    leaving = []

    def exchange(stage, src, dst, size, over_z, relay=None):
        me = a if over_z else b
        peers = peers_z if over_z else peers_y
        whole = pl.ds(0, (NPEER - 1) * size)

        def rows_of(index):
            return pl.ds(pl.multiple_of(index * size, 8), size)

        def copy(source, target, peer, send_sem, recv_sem):
            return pltpu.make_async_remote_copy(
                src_ref=source,
                dst_ref=target,
                send_sem=send_sem,
                recv_sem=recv_sem,
                device_id=(peer, b) if over_z else (a, peer),
                device_id_type=MESH,
            )

        send_sem, recv_sem = send_sems.at[stage], recv_sems.at[stage]
        passing = []
        if relay is not None:
            buffer, sems = relay
            step = (a // 2 + 6) % 8 * 2
            origin = (a // 2 + 2) % 8 * 2 + a % 2
            for k in range(2):
                held = buffer.at[pl.ds(k * size, size), :]
                copy(
                    src.at[rows_of(peers[k]), :], held, step + a % 2, send_sem, relay_sems.at[sems]
                ).start()
                passing.append(
                    copy(
                        held,
                        dst.at[rows_of(origin), :],
                        step + (a + 1 - k) % 2,
                        relay_sems.at[sems + 1],
                        recv_sem,
                    )
                )
            peers = peers[2:]
        for peer in peers:
            copy(src.at[rows_of(peer), :], dst.at[rows_of(me), :], peer, send_sem, recv_sem).start()
        dst[rows_of(me), :] = src[rows_of(me), :]
        every = copy(src.at[whole, :], dst.at[whole, :], peers[0], send_sem, recv_sem)
        leaving.append(every.wait_send)
        if relay is not None:
            both = pl.ds(0, 2 * size)
            held = copy(
                buffer.at[both, :],
                buffer.at[both, :],
                peers[0],
                relay_sems.at[sems + 1],
                relay_sems.at[sems],
            )
            leaving.append(held.wait_send)

            def forward():
                held.wait_recv()
                for message in passing:
                    message.start()

            return every.wait_recv, forward
        return every.wait_recv

    def rim_copy(index, source, target, peer):
        return pltpu.make_async_remote_copy(
            src_ref=source,
            dst_ref=target,
            send_sem=rim_sems.at[2 * index],
            recv_sem=rim_sems.at[2 * index + 1],
            device_id=peer,
            device_id_type=MESH,
        )

    rims = [
        rim_copy(k, tile_ref.at[pl.ds(first, size), :], rim_in.at[pl.ds(first - 256, size), :], peer)
        for k, (first, size, peer) in enumerate(
            ((368, 16, (after_z, after)), (256, 64, (after_z, b)), (320, 48, (a, after)))
        )
    ]
    for copy in rims:
        copy.start()

    def transform_x(value):
        high, low = split(value)
        return nn_dot(high, fx[0]) + nn_dot(high, fx[1]) + nn_dot(low, fx[0])

    spectrum = transform_x(tile_ref[0:256, :])
    for copy in rims:
        copy.wait()
    extra = transform_x(rim_in[...])
    iota = lax.broadcasted_iota(jnp.int32, (8, 256), 0)
    planes = [spectrum[16 * y : 16 * y + 16] for y in range(16)]
    for y in range(16):
        halo = extra[8 * (y // 2) : 8 * (y // 2) + 8]
        if y < 4:
            halo = halo + extra[112 + 8 * (y // 2) : 120 + 8 * (y // 2)]
        halo = jnp.where(iota < 4, halo if y % 2 == 0 else pltpu.roll(halo, 4, 0), 0.0)
        plane = jnp.concatenate([planes[y][:8] + halo, planes[y][8:]], 0)
        planes[y] = plane + extra[64 + 16 * y : 80 + 16 * y] if y < 3 else plane

    def send_lines(stream):
        lanes = slice(128 * stream, 128 * stream + 128)
        for peer, piece in enumerate(turn([plane[:, lanes] for plane in planes])):
            first = 256 * stream + 16 * peer
            send_1[first : first + 16, :] = piece

    def part(ref, stream):
        return ref.at[pl.ds(256 * stream, 256), :]

    send_lines(0)
    arrive_10 = exchange(0, part(send_1, 0), part(recv_1, 0), 16, True)
    send_lines(1)
    arrive_11, forward = exchange(1, part(send_1, 1), part(recv_1, 1), 16, True, (held_1, 0))
    tables_of_influence(
        moduli_ref, screening_ref[0], a, b, (straight_0, straight_1, crossed_0)
    )
    forward()

    half = lax.broadcasted_iota(jnp.int32, (1, 128), 1) < 64
    forward_sign = jnp.where(half, 1.0, -1.0)

    def product(table, value):
        high, low = split(value)
        width = value.shape[1]
        both = nn_dot(table[0], jnp.concatenate([high, low], 1))
        return both[:, :width] + both[:, width:] + nn_dot(table[1], high)

    def joined(both, sign):
        rows = both.shape[0] // 2
        return both[:rows] + wide(sign, rows) * pltpu.roll(both[rows:], 64, 1)

    def stage_z(stream):
        lines = recv_1[256 * stream : 256 * stream + 256, :]
        waves = joined(product(fz, lines), forward_sign)
        turned = turn([waves[16 * k : 16 * k + 16] for k in range(16)])
        for y in range(16):
            send_2[pl.ds(256 * stream + y, 16, stride=16), :] = turned[y]
        return exchange(2 + stream, part(send_2, stream), part(recv_2, stream), 16, False)

    def stage_y(stream):
        lines = recv_2[256 * stream : 256 * stream + 256, :]
        if stream == 0:
            lane = lax.broadcasted_iota(jnp.int32, (256, 128), 1)
            odd = (lane >> 2) & 1
            swapped = jnp.where(odd == 0, pltpu.roll(lines, 124, 1), pltpu.roll(lines, 4, 1))
            own_pair = wide(((lax.broadcasted_iota(jnp.int32, (1, 128), 1) & 63) >> 3) + b, 256) == 0
            swapped = jnp.where(own_pair, lines, swapped)
            both = product(fy, jnp.concatenate([lines, swapped * wide(forward_sign, 256)], 1))
            waves = joined(both[:, :128], forward_sign) * straight_0[...]
            waves = waves + joined(both[:, 128:], forward_sign) * crossed_0[...]
        else:
            waves = joined(product(fy, lines), forward_sign) * straight_1[...]
        first = 256 * stream
        send_3[first : first + 256, :] = joined(product(fy, waves), -forward_sign)
        return exchange(4 + stream, part(send_3, stream), part(recv_3, stream), 16, False)

    def stage_z_back(stream):
        pieces = [recv_3[pl.ds(256 * stream + y, 16, stride=16), :] for y in range(16)]
        lines = jnp.concatenate(turn(pieces), 0)
        first = 256 * stream
        send_4[first : first + 256, :] = joined(product(gz, lines), -forward_sign)
        relay = (held_4, 2) if stream else None
        return exchange(6 + stream, part(send_4, stream), part(recv_4, stream), 16, True, relay)

    arrive_10()
    arrive_20 = stage_z(0)
    arrive_11()
    arrive_21 = stage_z(1)
    arrive_20()
    arrive_30 = stage_y(0)
    arrive_21()
    arrive_31 = stage_y(1)
    arrive_30()
    arrive_40 = stage_z_back(0)
    arrive_31()
    arrive_41, forward = stage_z_back(1)
    handed_first(
        live, kept, charge_ref, frac_ref, cell_ref, charge_in_order, frac_in_order, cell_in_order
    )
    forward()
    def lines_back(stream):
        return turn(
            [recv_4[256 * stream + 16 * k : 256 * stream + 16 * k + 16, :] for k in range(16)]
        )

    arrive_40()
    turned_0 = lines_back(0)
    arrive_41()
    turned_1 = lines_back(1)

    high, low = split(
        jnp.concatenate([jnp.concatenate(pair, 1) for pair in zip(turned_0, turned_1)], 0)
    )
    value = nn_dot(high, gx[0]) + nn_dot(high, gx[1]) + nn_dot(low, gx[0])
    pot_ref[0:256, :] = value
    for pair in range(8):
        even, odd = value[32 * pair : 32 * pair + 8], value[32 * pair + 16 : 32 * pair + 24]
        planes_out[8 * pair : 8 * pair + 8, :] = jnp.where(iota < 4, even, pltpu.roll(odd, 4, 0))
    copies = [
        rim_copy(3 + k, source.at[pl.ds(0, size), :], pot_ref.at[pl.ds(target, size), :], peer)
        for k, (source, target, size, peer) in enumerate(
            (
                (planes_out, 368, 16, (before_z, before)),
                (planes_out, 256, 64, (before_z, b)),
                (pot_ref, 320, 48, (a, before)),
            )
        )
    ]
    for copy in copies:
        copy.start()
    for leave in leaving:
        leave()

    def keep_parts(rows):
        high, low = split(pot_ref[rows, :])
        p_hi[rows, :] = high
        p_lo[rows, :] = low

    def compute(*split_of, after_first=None):
        atoms = (charge_in_order, frac_in_order, cell_in_order)
        gather_atoms(*split_of, *atoms, forces, p_hi, p_lo, after_first)

    hand_on = rim_copy(6, forces.at[:, pl.ds(0, SEND_MAX * BLOCK)], guests, (a, after))
    keep_parts(slice(0, CORE))
    compute((0, EARLY), True, False)
    for copy in copies:
        copy.wait()
    keep_parts(slice(CORE, ROWS))
    compute((0, EARLY), False, True)
    compute((EARLY, ATOMS_DEV // CHUNK), True, True, after_first=hand_on.start)
    hand_on.wait()
    place_forces(kept, kept_before, arriving, forces, guests, out_ref)


def solve(live_blocks, send_blocks, screening, charge, fractions, cells, moduli):
    tables = []
    for table in (forward_x(), inverse_x(), *tables_z(), table_y()):
        tables.append(jnp.asarray(np.stack(split_np(table))))
    short, both = pltpu.VMEM((256, 128), F32), pltpu.VMEM((512, 128), F32)
    return pl.pallas_call(
        solve_kernel,
        out_shape=jax.ShapeDtypeStruct((3, ATOMS_DEV), F32),
        in_specs=[pl.BlockSpec(memory_space=pltpu.SMEM)] * 3
        + [pl.BlockSpec(memory_space=pltpu.VMEM)] * 4
        + [pl.BlockSpec(memory_space=pltpu.HBM)] * len(tables),
        out_specs=pl.BlockSpec(memory_space=pltpu.VMEM),
        scratch_shapes=[pltpu.VMEM(table.shape, BF16) for table in tables]
        + [pltpu.SemaphoreType.DMA((len(tables),))]
        + [pltpu.VMEM((ROWS, GRID), F32)] * 2
        + [pltpu.VMEM((128, GRID), F32), pltpu.VMEM((64, GRID), F32)]
        + [both] * 8
        + [short] * 3
        + [pltpu.VMEM((ROWS, GRID), BF16)] * 2
        + [
            pltpu.VMEM((3, ATOMS_DEV), F32),
            pltpu.VMEM((3, SEND_MAX * BLOCK), F32),
            pltpu.VMEM((1, ATOMS_DEV), F32),
            pltpu.VMEM((3, ATOMS_DEV), F32),
            pltpu.VMEM((3, ATOMS_DEV), jnp.int32),
            pltpu.VMEM((32, 128), F32),
            pltpu.VMEM((32, 128), F32),
            pltpu.SemaphoreType.DMA((14,)),
            pltpu.SemaphoreType.DMA((4,)),
            pltpu.SemaphoreType.DMA((8,)),
            pltpu.SemaphoreType.DMA((8,)),
        ],
        compiler_params=pltpu.CompilerParams(collective_id=0, has_side_effects=True),
        name="forces",
    )(live_blocks, send_blocks, screening, charge, fractions, cells, moduli, *tables)


def body(charge, fractions, cell_base, live_blocks, send_blocks, moduli, screening):
    return solve(
        live_blocks, send_blocks, screening, charge[None, :], fractions, cell_base, moduli
    )


def solution(mesh):
    return jax.shard_map(
        body,
        mesh=mesh,
        in_specs=(
            P(("gz", "gy")),
            P(None, ("gz", "gy")),
            P(None, ("gz", "gy")),
            P("gz", None),
            P("gz", None),
            P(),
            P(),
        ),
        out_specs=P(None, ("gz", "gy")),
        check_vma=False,
    )
```

```python
import functools

import jax
import jax.numpy as jnp
import numpy as np
from jax import lax
from jax.experimental import pallas as pl
from jax.experimental.pallas import tpu as pltpu
from jax.sharding import PartitionSpec as P

GRID = 256
BLOCK = 128
ATOMS_DEV = 12288
NBLK = 96
SEND_MAX = 36
NPEER = 16
CHUNK = 512
SPREAD_UNROLL = 4
GATHER_UNROLL = 4
EARLY = 8
CORE = 256
ROWS = 384
MESH = pl.DeviceIdType.MESH
BF16 = jnp.bfloat16
F32 = jnp.float32


def split_np(table):
    table = np.asarray(table, np.float32)
    high = table.astype(jnp.bfloat16)
    low = (table - high.astype(np.float32)).astype(jnp.bfloat16)
    return high, low


def kz_of(block, local):
    j = 8 * block + local // 2
    return np.where(local % 2 == 0, j, np.where(j == 0, 128, (256 - j) % 256))


def kx_order():
    stream, block, j = np.meshgrid(np.arange(2), np.arange(16), np.arange(4), indexing="ij")
    return (8 * block + 4 * stream + j).reshape(2, 64)


def forward_x():
    x = np.arange(256)[:, None]
    columns = []
    for kx in kx_order():
        angle = 2 * np.pi * ((x * kx[None, :]) % 256) / 256
        last = np.where(kx[None, :] == 0, (-1.0) ** x, -np.sin(angle))
        columns += [np.cos(angle), last]
    return np.concatenate(columns, 1)


def inverse_x():
    x = np.arange(256)[None, :]
    rows = []
    for kx in kx_order():
        angle = 2 * np.pi * ((x * kx[:, None]) % 256) / 256
        first = np.where(kx[:, None] == 0, 1.0, 2 * np.cos(angle))
        last = np.where(kx[:, None] == 0, (-1.0) ** x, -2 * np.sin(angle))
        rows += [first, last]
    return np.concatenate(rows, 0) / 256


def cos_sin(first, second):
    angle = 2 * np.pi * ((first[:, None] * second[None, :]) % 256) / 256
    return np.cos(angle), np.sin(angle)


def tables_z():
    local, block = np.meshgrid(np.arange(16), np.arange(16), indexing="ij")
    parts = cos_sin(kz_of(block, local).reshape(-1), np.arange(256))
    return np.concatenate(parts, 0), np.concatenate([part.T for part in parts], 0)


def table_y():
    return np.concatenate(cos_sin(np.arange(256), np.arange(256)), 0)


def split(value):
    high = value.astype(BF16)
    low = (value - high.astype(F32)).astype(BF16)
    return high, low


def spline_weights(t):
    remain = 1.0 - t
    square = t * t
    cubed = square * t
    sixth = 1.0 / 6.0
    weights = [
        remain * remain * remain * sixth,
        (3.0 * cubed - 6.0 * square + 4.0) * sixth,
        (-3.0 * cubed + 3.0 * square + 3.0 * t + 1.0) * sixth,
        cubed * sixth,
    ]
    return weights


def spline_slopes(t):
    remain = 1.0 - t
    square = t * t
    return [
        -0.5 * remain * remain,
        1.5 * square - 2.0 * t,
        -1.5 * square + t + 0.5,
        0.5 * square,
    ]


def wide(row, count):
    return jnp.broadcast_to(row, (count, row.shape[1]))


def stencil(offset, cell, weights):
    rows = offset.shape[0]
    place = offset - wide(cell, rows)
    table = jnp.zeros(offset.shape, F32)
    for k in range(3, -1, -1):
        table = jnp.where(place == k, wide(weights[k], rows), table)
    return table


def narrow_tables(cells, weights, row):
    cell = cells[row : row + 1]
    picked = [w[row : row + 1] for w in weights]
    iota = lax.broadcasted_iota(jnp.int32, (16, cell.shape[1]), 0)
    return stencil(iota, cell, picked), stencil(16 + (iota[:8] & 3), cell, picked)


def x_tables(cells, weight_sets):
    cell = cells[2:3]
    keys = [wide(((cell + m) & 255).astype(F32), 16).astype(BF16) for m in range(4)]
    sets = [[wide(w, 16).astype(BF16) for w in weights] for weights in weight_sets]
    base = lax.broadcasted_iota(jnp.int32, (16, 128), 0).astype(F32)
    results = [[] for _ in sets]
    for tile in range(16):
        place = (base + float(16 * tile)).astype(BF16)
        tables = [jnp.zeros((16, 128), BF16) for _ in sets]
        for m in range(3, -1, -1):
            hit = place == keys[m]
            tables = [jnp.where(hit, weights[m], t) for weights, t in zip(sets, tables)]
        for result, table in zip(results, tables):
            result.append(table)
    return [jnp.concatenate(result, 0) for result in results]


def high_low(rows):
    high = [w.astype(BF16).astype(F32) for w in rows]
    return high, [w - h for w, h in zip(rows, high)]


def nt_dot(a, b):
    return lax.dot_general(a, b, (((1,), (1,)), ((), ())), preferred_element_type=F32)


def nn_dot(a, b):
    return lax.dot_general(a, b, (((1,), (0,)), ((), ())), preferred_element_type=F32)


def tn_dot(a, b):
    return lax.dot_general(a, b, (((0,), (0,)), ((), ())), preferred_element_type=F32)


def pair_pattern(table, pair):
    iota = lax.broadcasted_iota(jnp.int32, (8, table.shape[1]), 0)
    return jnp.where(
        iota < 4, wide(table[2 * pair : 2 * pair + 1], 8), wide(table[2 * pair + 1 : 2 * pair + 2], 8)
    )


def plane_tables(cells, weights):
    z_main, z_halo = narrow_tables(cells, weights, 0)
    y_main, y_halo = narrow_tables(cells, weights, 1)
    pieces = [wide(y_main[y : y + 1], 16) * z_main for y in range(16)]
    pieces += [pair_pattern(y_main, pair) * z_halo for pair in range(8)]
    pieces += [wide(y_halo[y : y + 1], 16) * z_main for y in range(3)]
    pieces += [pair_pattern(y_halo, pair) * z_halo for pair in range(2)]
    return split(jnp.concatenate(pieces, 0))


def spread_atoms(live, charge_ref, frac_ref, cell_ref, tile_ref):
    n = CHUNK
    tile_ref[...] = jnp.zeros_like(tile_ref)

    def chunk(first):
        q_all = charge_ref[:, pl.ds(first, n)]
        lanes = first + lax.broadcasted_iota(jnp.int32, (1, n), 1)
        q_all = jnp.where(lanes < live, q_all, 0.0)
        weights_all = spline_weights(frac_ref[:, pl.ds(first, n)])
        cells_all = cell_ref[:, pl.ds(first, n)]
        columns = []
        for group in range(n // 128):
            lanes = slice(128 * group, 128 * group + 128)
            weights = [w[:, lanes] for w in weights_all]
            cells, q = cells_all[:, lanes], q_all[:, lanes]
            columns.append(
                tuple(x_tables(cells, high_low([w[2:3] * q for w in weights])))
                + plane_tables(cells, weights)
            )
        x_hi, x_lo, a_hi, a_lo = (jnp.concatenate(part, 1) for part in zip(*columns))
        tile_ref[...] += nt_dot(a_hi, x_hi) + nt_dot(a_hi, x_lo) + nt_dot(a_lo, x_hi)

    def step(i, carry):
        for u in range(SPREAD_UNROLL):
            chunk(pl.multiple_of((SPREAD_UNROLL * i + u) * n, n))
        return carry

    lax.fori_loop(0, ATOMS_DEV // (n * SPREAD_UNROLL), step, 0)


def wide_x_tables(cells, weights, slopes):
    columns = []
    for group in range(cells.shape[1] // 128):
        lanes = slice(128 * group, 128 * group + 128)
        columns.append(
            x_tables(
                cells[:, lanes],
                high_low([w[2:3, lanes] for w in weights])
                + high_low([w[2:3, lanes] for w in slopes]),
            )
        )
    return [jnp.concatenate(part, 1) for part in zip(*columns)]


def hold_x_tables(frac_ref, cell_ref, held):
    def step(index, carry):
        place = pl.ds(pl.multiple_of(index * 256, 256), 256)
        t = frac_ref[:, place]
        tables = wide_x_tables(cell_ref[:, place], spline_weights(t), spline_slopes(t))
        for k, table in enumerate(tables):
            held[k, index] = table
        return carry

    lax.fori_loop(0, EARLY * CHUNK // 256, step, 0)


def gather_atoms(
    chunks, own, rim, charge_ref, frac_ref, cell_ref, out_ref, p_hi, p_lo, held=None, after_first=None
):
    base = 0 if own else CORE
    rows = slice(base, ROWS if rim else CORE)
    n = 256

    def piece_of(index):
        first = pl.multiple_of(index * n, n)
        t = frac_ref[:, pl.ds(first, n)]
        cells_all = cell_ref[:, pl.ds(first, n)]
        weights_all, slopes_all = spline_weights(t), spline_slopes(t)
        if held is None:
            w_hi, w_lo, s_hi, s_lo = wide_x_tables(cells_all, weights_all, slopes_all)
        else:
            w_hi, w_lo, s_hi, s_lo = (held[k, index] for k in range(4))
        hi, lo = p_hi[rows, :], p_lo[rows, :]
        along_all = nn_dot(hi, w_hi) + nn_dot(hi, w_lo) + nn_dot(lo, w_hi)
        steep_all = nn_dot(hi, s_hi) + nn_dot(hi, s_lo) + nn_dot(lo, s_hi)
        results = []
        for group in range(n // 128):
            lanes = slice(128 * group, 128 * group + 128)
            along, steep = along_all[:, lanes], steep_all[:, lanes]
            weights = [w[:, lanes] for w in weights_all]
            slopes = [w[:, lanes] for w in slopes_all]
            cells = cells_all[:, lanes]
            zw_main, zw_halo = narrow_tables(cells, weights, 0)
            zs_main, zs_halo = narrow_tables(cells, slopes, 0)
            yw_main, yw_halo = narrow_tables(cells, weights, 1)
            ys_main, ys_halo = narrow_tables(cells, slopes, 1)
            sums = [jnp.zeros((16, 128), F32)] * 3
            for y in range(0 if own else 16, 19 if rim else 16):
                row = 16 * y if y < 16 else 320 + 16 * (y - 16) - base
                yw = wide(yw_main[y : y + 1] if y < 16 else yw_halo[y - 16 : y - 15], 16)
                ys = wide(ys_main[y : y + 1] if y < 16 else ys_halo[y - 16 : y - 15], 16)
                piece, slope = along[row : row + 16], steep[row : row + 16]
                sums = [sums[0] + yw * piece, sums[1] + ys * piece, sums[2] + yw * slope]
            rims = [jnp.zeros((8, 128), F32)] * 3
            for pair in range(10 if rim else 0):
                row = (256 + 8 * pair if pair < 8 else 368 + 8 * (pair - 8)) - base
                yw = pair_pattern(yw_main, pair) if pair < 8 else pair_pattern(yw_halo, pair - 8)
                ys = pair_pattern(ys_main, pair) if pair < 8 else pair_pattern(ys_halo, pair - 8)
                piece, slope = along[row : row + 8], steep[row : row + 8]
                rims = [rims[0] + yw * piece, rims[1] + ys * piece, rims[2] + yw * slope]
            sums = [sums[0] * zs_main, sums[1] * zw_main, sums[2] * zw_main]
            rims = [rims[0] * zs_halo, rims[1] * zw_halo, rims[2] * zw_halo]
            results.append(
                jnp.concatenate(
                    [
                        jnp.sum(f[:8] + f[8:] + r, axis=0, keepdims=True)
                        for f, r in zip(sums, rims)
                    ],
                    0,
                )
            )
        q = charge_ref[:, pl.ds(first, n)]
        result = jnp.concatenate(results, 1) * -q
        if not own:
            result = result + out_ref[:, pl.ds(first, n)]
        out_ref[:, pl.ds(first, n)] = result

    low, high = chunks
    per_step = GATHER_UNROLL * CHUNK

    def step(i, carry):
        for u in range(per_step // n):
            piece_of(low * (CHUNK // n) + i * (per_step // n) + u)
        if after_first is not None:
            pl.when(i == 0)(after_first)
        return carry

    lax.fori_loop(0, (high - low) // GATHER_UNROLL, step, 0)


def turn(arrays):
    arrays = list(arrays)
    rows = arrays[0].shape[0]
    group = lax.broadcasted_iota(jnp.int32, (rows, 128), 1) >> 2
    for bit in range(4):
        g = 1 << bit
        keep = (group & g) == 0
        fresh = list(arrays)
        for i in range(16):
            if i & g == 0:
                low, high = arrays[i], arrays[i | g]
                fresh[i] = jnp.where(keep, low, pltpu.roll(high, 4 * g, 1))
                fresh[i | g] = jnp.where(keep, pltpu.roll(low, 128 - 4 * g, 1), high)
        arrays = fresh
    return arrays


def tables_of_influence(moduli_ref, screening, a, b, outs):
    m = [moduli_ref[c : c + 1, :] for c in range(3)]
    lane_k = lax.broadcasted_iota(jnp.int32, (256, 256), 1)
    row_k = lax.broadcasted_iota(jnp.int32, (256, 256), 0)
    same = lane_k == row_k
    other = lane_k == ((256 - row_k) & 255)

    def column(row, mask):
        return jnp.sum(jnp.where(mask, wide(row, 256), 0.0), axis=1, keepdims=True)

    m0, m1, m2 = column(m[0], same), column(m[1], same), column(m[2], same)
    m1_back = column(m[1], other)

    lane = lax.broadcasted_iota(jnp.int32, (1, 128), 1)
    local, j = (lane >> 2) & 15, lane & 3
    step = 8 * b + (local >> 1)
    kz = jnp.where(local & 1 == 0, step, jnp.where(step == 0, 128, 256 - step))
    rows = lax.broadcasted_iota(jnp.int32, (256, 128), 0)

    def along_lanes(col, index):
        hit = rows == wide(index, 256)
        return jnp.sum(jnp.where(hit, jnp.broadcast_to(col, (256, 128)), 0.0), 0, keepdims=True)

    z0, z1 = along_lanes(m0, kz), along_lanes(m0, (256 - kz) & 255)
    def signed(k):
        return jnp.where(k < 128, k, k - 256)

    nz, ny = signed(kz), signed(rows)
    flat = ny * ny + wide(nz * nz, 256)

    def kernel_at(kx):
        nx = signed(kx)
        radius = flat + wide(nx * nx, 256)
        squared = radius.astype(F32) / float(GRID * GRID)
        safe = jnp.where(radius > 0, squared, 1.0)
        first, second = along_lanes(m2, kx), along_lanes(m2, (256 - kx) & 255)
        product = m1 * wide(z0 * first, 256) + m1_back * wide(z1 * second, 256)
        value = product * jnp.exp(-screening * squared) / safe
        return jnp.where(radius > 0, value, 0.0) * (1.0 / float(GRID * GRID))

    kx = 8 * a + j
    at_first, at_last = kernel_at(kx), kernel_at(jnp.full_like(kx, 128))
    packed = wide(kx, 256) == 0
    outs[0][...] = jnp.where(packed, 0.5 * (at_first + at_last), at_first)
    outs[1][...] = kernel_at(kx + 4)
    outs[2][...] = jnp.where(packed, 0.5 * (at_first - at_last), 0.0)


def block(ref, index):
    return ref[:, BLOCK * index : BLOCK * index + BLOCK]


def shift_left(blocks, amount, top, keep):
    bit = top
    while bit:
        take = wide((amount & bit) > 0, blocks[0].shape[0])
        count = min(len(blocks), keep + bit - 1)
        last = len(blocks) - 1
        blocks = [
            jnp.where(take, blocks[min(i + bit, last)], blocks[i]) for i in range(count)
        ]
        bit //= 2
    return blocks


def handed_first(live, kept, charge_ref, frac_ref, cell_ref, charge_out, frac_out, cell_out):
    home = NBLK - SEND_MAX
    start = jnp.minimum(jnp.full((1, BLOCK), kept, jnp.int32), home)
    count = jnp.full((1, BLOCK), live, jnp.int32)
    charges = [jnp.where(count > i, block(charge_ref, i), 0.0) for i in range(NBLK)]
    for blocks, out in (
        (charges, charge_out),
        ([block(frac_ref, i) for i in range(NBLK)], frac_out),
        ([block(cell_ref, i) for i in range(NBLK)], cell_out),
    ):
        ordered = shift_left(blocks, start, 32, SEND_MAX) + blocks[:home]
        for i, value in enumerate(ordered):
            out[:, BLOCK * i : BLOCK * i + BLOCK] = value


def place_forces(kept, kept_before, arriving, forces, guests, out_ref):
    home = NBLK - SEND_MAX
    kept = jnp.full((1, BLOCK), kept, jnp.int32)
    kept_before = jnp.full((1, BLOCK), kept_before, jnp.int32)
    end = kept + arriving
    skip = kept_before - jnp.minimum(kept_before, home)
    arrived = shift_left([block(guests, i) for i in range(SEND_MAX)], skip, 32, SEND_MAX)
    placed = arrived + [jnp.zeros((3, BLOCK), F32)] * (NBLK - SEND_MAX)
    bit = 64
    while bit:
        take = wide((kept & bit) > 0, 3)
        placed = [
            jnp.where(take, placed[i - bit] if i >= bit else 0.0, placed[i]) for i in range(NBLK)
        ]
        bit //= 2
    for slot in range(NBLK):
        own = block(forces, SEND_MAX + slot if slot < home else slot - home)
        guest = jnp.where(wide(end > slot, 3), placed[slot], 0.0)
        out_ref[:, BLOCK * slot : BLOCK * slot + BLOCK] = jnp.where(wide(kept > slot, 3), own, guest)


def offsets_z():
    return [(dz, dy) for dz in (4, 3, -3, 2, -2, 1, -1, 0) for dy in (1, 0) if (dz, dy) != (0, 0)]


def offsets_y():
    moves = [(dx, dy, dc) for dx in (2, 1, -1, 0) for dy in (1, 0) for dc in (1, 0)]
    moves.remove((0, 0, 0))
    return sorted(moves, key=lambda m: -(abs(m[0]) + 2 * m[1]))


def solve_kernel(
    live_ref,
    send_ref,
    screening_ref,
    charge_ref,
    frac_ref,
    cell_ref,
    moduli_ref,
    fx_far,
    gx_far,
    fz_far,
    gz_far,
    fy_far,
    out_ref,
    fx,
    gx,
    fz,
    gz,
    fy,
    table_sems,
    tile_ref,
    pot_ref,
    rim_in,
    planes_out,
    send_1,
    recv_1,
    send_2,
    recv_2,
    send_3,
    recv_3,
    send_4,
    recv_4,
    straight_0,
    straight_1,
    crossed_0,
    p_hi,
    p_lo,
    forces,
    guests,
    charge_in_order,
    frac_in_order,
    cell_in_order,
    held,
    held_1,
    held_4,
    rim_sems,
    relay_sems,
    send_sems,
    recv_sems,
):
    a, b = lax.axis_index("gz"), lax.axis_index("gy")
    barrier = pltpu.get_barrier_semaphore()
    peers_z = [
        ((a // 2 + dz + 8) % 8) * 2 + (a + dy) % 2 for dz, dy in offsets_z()
    ]
    peers_y = [
        ((b // 4 + dx + 4) % 4) * 4 + ((b // 2 + dy) % 2) * 2 + (b + dc) % 2
        for dx, dy, dc in offsets_y()
    ]
    for peer in peers_z:
        pl.semaphore_signal(barrier, inc=1, device_id=(peer, b), device_id_type=MESH)
    for peer in peers_y:
        pl.semaphore_signal(barrier, inc=1, device_id=(a, peer), device_id_type=MESH)

    loads = [
        pltpu.make_async_copy(far, near, table_sems.at[k])
        for k, (far, near) in enumerate(
            ((fx_far, fx), (fz_far, fz), (fy_far, fy), (gz_far, gz), (gx_far, gx))
        )
    ]
    for load in loads:
        load.start()

    before, after = (b + 15) % 16, (b + 1) % 16
    before_z, after_z = (a + 15) % 16, (a + 1) % 16
    for peer in ((before_z, before), (after_z, after)):
        pl.semaphore_signal(barrier, inc=1, device_id=peer, device_id_type=MESH)
    live = live_ref[0, b]
    kept = live - send_ref[0, b]
    kept_before = live_ref[0, before] - send_ref[0, before]
    arriving = send_ref[0, before]
    spread_atoms(live * BLOCK, charge_ref, frac_ref, cell_ref, tile_ref)
    for load in loads:
        load.wait()
    pl.semaphore_wait(barrier, 2 * NPEER)

    leaving = []

    def exchange(stage, src, dst, size, over_z, relay=None):
        me = a if over_z else b
        peers = peers_z if over_z else peers_y
        whole = pl.ds(0, (NPEER - 1) * size)

        def rows_of(index):
            return pl.ds(pl.multiple_of(index * size, 8), size)

        def copy(source, target, peer, send_sem, recv_sem):
            return pltpu.make_async_remote_copy(
                src_ref=source,
                dst_ref=target,
                send_sem=send_sem,
                recv_sem=recv_sem,
                device_id=(peer, b) if over_z else (a, peer),
                device_id_type=MESH,
            )

        send_sem, recv_sem = send_sems.at[stage], recv_sems.at[stage]
        passing = []
        if relay is not None:
            buffer, sems = relay
            step = (a // 2 + 6) % 8 * 2
            origin = (a // 2 + 2) % 8 * 2 + a % 2
            for k in range(2):
                leg = buffer.at[pl.ds(k * size, size), :]
                copy(
                    src.at[rows_of(peers[k]), :], leg, step + a % 2, send_sem, relay_sems.at[sems]
                ).start()
                passing.append(
                    copy(
                        leg,
                        dst.at[rows_of(origin), :],
                        step + (a + 1 - k) % 2,
                        relay_sems.at[sems + 1],
                        recv_sem,
                    )
                )
            peers = peers[2:]
        for peer in peers:
            copy(src.at[rows_of(peer), :], dst.at[rows_of(me), :], peer, send_sem, recv_sem).start()
        dst[rows_of(me), :] = src[rows_of(me), :]
        every = copy(src.at[whole, :], dst.at[whole, :], peers[0], send_sem, recv_sem)
        leaving.append(every.wait_send)
        if relay is not None:
            both = pl.ds(0, 2 * size)
            legs = copy(
                buffer.at[both, :],
                buffer.at[both, :],
                peers[0],
                relay_sems.at[sems + 1],
                relay_sems.at[sems],
            )
            leaving.append(legs.wait_send)

            def forward():
                legs.wait_recv()
                for message in passing:
                    message.start()

            return every.wait_recv, forward
        return every.wait_recv

    def rim_copy(index, source, target, peer):
        return pltpu.make_async_remote_copy(
            src_ref=source,
            dst_ref=target,
            send_sem=rim_sems.at[2 * index],
            recv_sem=rim_sems.at[2 * index + 1],
            device_id=peer,
            device_id_type=MESH,
        )

    rims = [
        rim_copy(k, tile_ref.at[pl.ds(first, size), :], rim_in.at[pl.ds(first - 256, size), :], peer)
        for k, (first, size, peer) in enumerate(
            ((368, 16, (after_z, after)), (256, 64, (after_z, b)), (320, 48, (a, after)))
        )
    ]
    for copy in rims:
        copy.start()

    def transform_x(value):
        high, low = split(value)
        return nn_dot(high, fx[0]) + nn_dot(high, fx[1]) + nn_dot(low, fx[0])

    spectrum = transform_x(tile_ref[0:256, :])
    handed_first(
        live, kept, charge_ref, frac_ref, cell_ref, charge_in_order, frac_in_order, cell_in_order
    )
    hold_x_tables(frac_in_order, cell_in_order, held)
    for copy in rims:
        copy.wait()
    extra = transform_x(rim_in[...])
    iota = lax.broadcasted_iota(jnp.int32, (8, 256), 0)
    planes = [spectrum[16 * y : 16 * y + 16] for y in range(16)]
    for y in range(16):
        halo = extra[8 * (y // 2) : 8 * (y // 2) + 8]
        if y < 4:
            halo = halo + extra[112 + 8 * (y // 2) : 120 + 8 * (y // 2)]
        halo = jnp.where(iota < 4, halo if y % 2 == 0 else pltpu.roll(halo, 4, 0), 0.0)
        plane = jnp.concatenate([planes[y][:8] + halo, planes[y][8:]], 0)
        planes[y] = plane + extra[64 + 16 * y : 80 + 16 * y] if y < 3 else plane

    def send_lines(stream):
        lanes = slice(128 * stream, 128 * stream + 128)
        for peer, piece in enumerate(turn([plane[:, lanes] for plane in planes])):
            first = 256 * stream + 16 * peer
            send_1[first : first + 16, :] = piece

    def part(ref, stream):
        return ref.at[pl.ds(256 * stream, 256), :]

    send_lines(0)
    arrive_10 = exchange(0, part(send_1, 0), part(recv_1, 0), 16, True)
    send_lines(1)
    arrive_11, forward = exchange(1, part(send_1, 1), part(recv_1, 1), 16, True, (held_1, 0))
    tables_of_influence(
        moduli_ref, screening_ref[0], a, b, (straight_0, straight_1, crossed_0)
    )
    forward()

    half = lax.broadcasted_iota(jnp.int32, (1, 128), 1) < 64
    forward_sign = jnp.where(half, 1.0, -1.0)

    def product(table, value):
        high, low = split(value)
        width = value.shape[1]
        both = nn_dot(table[0], jnp.concatenate([high, low], 1))
        return both[:, :width] + both[:, width:] + nn_dot(table[1], high)

    def joined(both, sign):
        rows = both.shape[0] // 2
        return both[:rows] + wide(sign, rows) * pltpu.roll(both[rows:], 64, 1)

    def stage_z(stream):
        lines = recv_1[256 * stream : 256 * stream + 256, :]
        waves = joined(product(fz, lines), forward_sign)
        turned = turn([waves[16 * k : 16 * k + 16] for k in range(16)])
        for y in range(16):
            send_2[pl.ds(256 * stream + y, 16, stride=16), :] = turned[y]
        return exchange(2 + stream, part(send_2, stream), part(recv_2, stream), 16, False)

    def stage_y(stream):
        lines = recv_2[256 * stream : 256 * stream + 256, :]
        if stream == 0:
            lane = lax.broadcasted_iota(jnp.int32, (256, 128), 1)
            odd = (lane >> 2) & 1
            swapped = jnp.where(odd == 0, pltpu.roll(lines, 124, 1), pltpu.roll(lines, 4, 1))
            own_pair = wide(((lax.broadcasted_iota(jnp.int32, (1, 128), 1) & 63) >> 3) + b, 256) == 0
            swapped = jnp.where(own_pair, lines, swapped)
            both = product(fy, jnp.concatenate([lines, swapped * wide(forward_sign, 256)], 1))
            waves = joined(both[:, :128], forward_sign) * straight_0[...]
            waves = waves + joined(both[:, 128:], forward_sign) * crossed_0[...]
        else:
            waves = joined(product(fy, lines), forward_sign) * straight_1[...]
        first = 256 * stream
        send_3[first : first + 256, :] = joined(product(fy, waves), -forward_sign)
        return exchange(4 + stream, part(send_3, stream), part(recv_3, stream), 16, False)

    def stage_z_back(stream):
        pieces = [recv_3[pl.ds(256 * stream + y, 16, stride=16), :] for y in range(16)]
        lines = jnp.concatenate(turn(pieces), 0)
        first = 256 * stream
        send_4[first : first + 256, :] = joined(product(gz, lines), -forward_sign)
        relay = (held_4, 2) if stream else None
        return exchange(6 + stream, part(send_4, stream), part(recv_4, stream), 16, True, relay)

    arrive_10()
    arrive_20 = stage_z(0)
    arrive_11()
    arrive_21 = stage_z(1)
    arrive_20()
    arrive_30 = stage_y(0)
    arrive_21()
    arrive_31 = stage_y(1)
    arrive_30()
    arrive_40 = stage_z_back(0)
    arrive_31()
    arrive_41, forward = stage_z_back(1)
    forward()
    def lines_back(stream):
        return turn(
            [recv_4[256 * stream + 16 * k : 256 * stream + 16 * k + 16, :] for k in range(16)]
        )

    arrive_40()
    turned_0 = lines_back(0)
    arrive_41()
    turned_1 = lines_back(1)

    high, low = split(
        jnp.concatenate([jnp.concatenate(pair, 1) for pair in zip(turned_0, turned_1)], 0)
    )
    value = nn_dot(high, gx[0]) + nn_dot(high, gx[1]) + nn_dot(low, gx[0])
    pot_ref[0:256, :] = value
    for pair in range(8):
        even, odd = value[32 * pair : 32 * pair + 8], value[32 * pair + 16 : 32 * pair + 24]
        planes_out[8 * pair : 8 * pair + 8, :] = jnp.where(iota < 4, even, pltpu.roll(odd, 4, 0))
    copies = [
        rim_copy(3 + k, source.at[pl.ds(0, size), :], pot_ref.at[pl.ds(target, size), :], peer)
        for k, (source, target, size, peer) in enumerate(
            (
                (planes_out, 368, 16, (before_z, before)),
                (planes_out, 256, 64, (before_z, b)),
                (pot_ref, 320, 48, (a, before)),
            )
        )
    ]
    for copy in copies:
        copy.start()
    for leave in leaving:
        leave()

    def keep_parts(rows):
        high, low = split(pot_ref[rows, :])
        p_hi[rows, :] = high
        p_lo[rows, :] = low

    def compute(*split_of, **options):
        atoms = (charge_in_order, frac_in_order, cell_in_order)
        gather_atoms(*split_of, *atoms, forces, p_hi, p_lo, **options)

    hand_on = rim_copy(6, forces.at[:, pl.ds(0, SEND_MAX * BLOCK)], guests, (a, after))
    keep_parts(slice(0, CORE))
    compute((0, EARLY), True, False, held=held)
    for copy in copies:
        copy.wait()
    keep_parts(slice(CORE, ROWS))
    compute((0, EARLY), False, True, held=held)
    compute((EARLY, ATOMS_DEV // CHUNK), True, True, after_first=hand_on.start)
    hand_on.wait()
    place_forces(kept, kept_before, arriving, forces, guests, out_ref)


def solve(live_blocks, send_blocks, screening, charge, fractions, cells, moduli):
    tables = []
    for table in (forward_x(), inverse_x(), *tables_z(), table_y()):
        tables.append(jnp.asarray(np.stack(split_np(table))))
    short, both = pltpu.VMEM((256, 128), F32), pltpu.VMEM((512, 128), F32)
    return pl.pallas_call(
        solve_kernel,
        out_shape=jax.ShapeDtypeStruct((3, ATOMS_DEV), F32),
        in_specs=[pl.BlockSpec(memory_space=pltpu.SMEM)] * 3
        + [pl.BlockSpec(memory_space=pltpu.VMEM)] * 4
        + [pl.BlockSpec(memory_space=pltpu.HBM)] * len(tables),
        out_specs=pl.BlockSpec(memory_space=pltpu.VMEM),
        scratch_shapes=[pltpu.VMEM(table.shape, BF16) for table in tables]
        + [pltpu.SemaphoreType.DMA((len(tables),))]
        + [pltpu.VMEM((ROWS, GRID), F32)] * 2
        + [pltpu.VMEM((128, GRID), F32), pltpu.VMEM((64, GRID), F32)]
        + [both] * 8
        + [short] * 3
        + [pltpu.VMEM((ROWS, GRID), BF16)] * 2
        + [
            pltpu.VMEM((3, ATOMS_DEV), F32),
            pltpu.VMEM((3, SEND_MAX * BLOCK), F32),
            pltpu.VMEM((1, ATOMS_DEV), F32),
            pltpu.VMEM((3, ATOMS_DEV), F32),
            pltpu.VMEM((3, ATOMS_DEV), jnp.int32),
            pltpu.VMEM((4, EARLY * CHUNK // 256, 256, 256), BF16),
            pltpu.VMEM((32, 128), F32),
            pltpu.VMEM((32, 128), F32),
            pltpu.SemaphoreType.DMA((14,)),
            pltpu.SemaphoreType.DMA((4,)),
            pltpu.SemaphoreType.DMA((8,)),
            pltpu.SemaphoreType.DMA((8,)),
        ],
        compiler_params=pltpu.CompilerParams(collective_id=0, has_side_effects=True),
        name="forces",
    )(live_blocks, send_blocks, screening, charge, fractions, cells, moduli, *tables)


def body(charge, fractions, cell_base, live_blocks, send_blocks, moduli, screening):
    return solve(
        live_blocks, send_blocks, screening, charge[None, :], fractions, cell_base, moduli
    )


def solution(mesh):
    return jax.shard_map(
        body,
        mesh=mesh,
        in_specs=(
            P(("gz", "gy")),
            P(None, ("gz", "gy")),
            P(None, ("gz", "gy")),
            P("gz", None),
            P("gz", None),
            P(),
            P(),
        ),
        out_specs=P(None, ("gz", "gy")),
        check_vma=False,
    )
```

```python
import functools

import jax
import jax.numpy as jnp
import numpy as np
from jax import lax
from jax.experimental import pallas as pl
from jax.experimental.pallas import tpu as pltpu
from jax.sharding import PartitionSpec as P

GRID = 256
BLOCK = 128
ATOMS_DEV = 12288
NBLK = 96
SEND_MAX = 36
NPEER = 16
CHUNK = 512
SPREAD_UNROLL = 4
GATHER_UNROLL = 4
EARLY = 12
CORE = 256
ROWS = 384
MESH = pl.DeviceIdType.MESH
BF16 = jnp.bfloat16
F32 = jnp.float32


def split_np(table):
    table = np.asarray(table, np.float32)
    high = table.astype(jnp.bfloat16)
    low = (table - high.astype(np.float32)).astype(jnp.bfloat16)
    return high, low


def kz_of(block, local):
    j = 8 * block + local // 2
    return np.where(local % 2 == 0, j, np.where(j == 0, 128, (256 - j) % 256))


def kx_order():
    stream, block, j = np.meshgrid(np.arange(2), np.arange(16), np.arange(4), indexing="ij")
    return (8 * block + 4 * stream + j).reshape(2, 64)


def forward_x():
    x = np.arange(256)[:, None]
    columns = []
    for kx in kx_order():
        angle = 2 * np.pi * ((x * kx[None, :]) % 256) / 256
        last = np.where(kx[None, :] == 0, (-1.0) ** x, -np.sin(angle))
        columns += [np.cos(angle), last]
    return np.concatenate(columns, 1)


def inverse_x():
    x = np.arange(256)[None, :]
    rows = []
    for kx in kx_order():
        angle = 2 * np.pi * ((x * kx[:, None]) % 256) / 256
        first = np.where(kx[:, None] == 0, 1.0, 2 * np.cos(angle))
        last = np.where(kx[:, None] == 0, (-1.0) ** x, -2 * np.sin(angle))
        rows += [first, last]
    return np.concatenate(rows, 0) / 256


def cos_sin(first, second):
    angle = 2 * np.pi * ((first[:, None] * second[None, :]) % 256) / 256
    return np.cos(angle), np.sin(angle)


def tables_z():
    local, block = np.meshgrid(np.arange(16), np.arange(16), indexing="ij")
    parts = cos_sin(kz_of(block, local).reshape(-1), np.arange(256))
    return np.concatenate(parts, 0), np.concatenate([part.T for part in parts], 0)


def table_y():
    return np.concatenate(cos_sin(np.arange(256), np.arange(256)), 0)


def split(value):
    high = value.astype(BF16)
    low = (value - high.astype(F32)).astype(BF16)
    return high, low


def spline_weights(t):
    remain = 1.0 - t
    square = t * t
    cubed = square * t
    sixth = 1.0 / 6.0
    weights = [
        remain * remain * remain * sixth,
        (3.0 * cubed - 6.0 * square + 4.0) * sixth,
        (-3.0 * cubed + 3.0 * square + 3.0 * t + 1.0) * sixth,
        cubed * sixth,
    ]
    return weights


def spline_slopes(t):
    remain = 1.0 - t
    square = t * t
    return [
        -0.5 * remain * remain,
        1.5 * square - 2.0 * t,
        -1.5 * square + t + 0.5,
        0.5 * square,
    ]


def wide(row, count):
    return jnp.broadcast_to(row, (count, row.shape[1]))


def stencil(offset, cell, weights):
    rows = offset.shape[0]
    place = offset - wide(cell, rows)
    table = jnp.zeros(offset.shape, F32)
    for k in range(3, -1, -1):
        table = jnp.where(place == k, wide(weights[k], rows), table)
    return table


def narrow_tables(cells, weights, row):
    cell = cells[row : row + 1]
    picked = [w[row : row + 1] for w in weights]
    iota = lax.broadcasted_iota(jnp.int32, (16, cell.shape[1]), 0)
    return stencil(iota, cell, picked), stencil(16 + (iota[:8] & 3), cell, picked)


def x_tables(cells, weight_sets):
    cell = cells[2:3]
    keys = [wide(((cell + m) & 255).astype(F32), 16).astype(BF16) for m in range(4)]
    sets = [[wide(w, 16).astype(BF16) for w in weights] for weights in weight_sets]
    base = lax.broadcasted_iota(jnp.int32, (16, 128), 0).astype(F32)
    results = [[] for _ in sets]
    for tile in range(16):
        place = (base + float(16 * tile)).astype(BF16)
        tables = [jnp.zeros((16, 128), BF16) for _ in sets]
        for m in range(3, -1, -1):
            hit = place == keys[m]
            tables = [jnp.where(hit, weights[m], t) for weights, t in zip(sets, tables)]
        for result, table in zip(results, tables):
            result.append(table)
    return [jnp.concatenate(result, 0) for result in results]


def high_low(rows):
    high = [w.astype(BF16).astype(F32) for w in rows]
    return high, [w - h for w, h in zip(rows, high)]


def nt_dot(a, b):
    return lax.dot_general(a, b, (((1,), (1,)), ((), ())), preferred_element_type=F32)


def nn_dot(a, b):
    return lax.dot_general(a, b, (((1,), (0,)), ((), ())), preferred_element_type=F32)


def tn_dot(a, b):
    return lax.dot_general(a, b, (((0,), (0,)), ((), ())), preferred_element_type=F32)


def pair_pattern(table, pair):
    iota = lax.broadcasted_iota(jnp.int32, (8, table.shape[1]), 0)
    return jnp.where(
        iota < 4, wide(table[2 * pair : 2 * pair + 1], 8), wide(table[2 * pair + 1 : 2 * pair + 2], 8)
    )


def plane_tables(cells, weights):
    z_main, z_halo = narrow_tables(cells, weights, 0)
    y_main, y_halo = narrow_tables(cells, weights, 1)
    pieces = [wide(y_main[y : y + 1], 16) * z_main for y in range(16)]
    pieces += [pair_pattern(y_main, pair) * z_halo for pair in range(8)]
    pieces += [wide(y_halo[y : y + 1], 16) * z_main for y in range(3)]
    pieces += [pair_pattern(y_halo, pair) * z_halo for pair in range(2)]
    return split(jnp.concatenate(pieces, 0))


def spread_atoms(live, charge_ref, frac_ref, cell_ref, tile_ref):
    n = CHUNK
    tile_ref[...] = jnp.zeros_like(tile_ref)

    def chunk(first):
        q_all = charge_ref[:, pl.ds(first, n)]
        lanes = first + lax.broadcasted_iota(jnp.int32, (1, n), 1)
        q_all = jnp.where(lanes < live, q_all, 0.0)
        weights_all = spline_weights(frac_ref[:, pl.ds(first, n)])
        cells_all = cell_ref[:, pl.ds(first, n)]
        columns = []
        for group in range(n // 128):
            lanes = slice(128 * group, 128 * group + 128)
            weights = [w[:, lanes] for w in weights_all]
            cells, q = cells_all[:, lanes], q_all[:, lanes]
            columns.append(
                tuple(x_tables(cells, high_low([w[2:3] * q for w in weights])))
                + plane_tables(cells, weights)
            )
        x_hi, x_lo, a_hi, a_lo = (jnp.concatenate(part, 1) for part in zip(*columns))
        tile_ref[...] += nt_dot(a_hi, x_hi) + nt_dot(a_hi, x_lo) + nt_dot(a_lo, x_hi)

    def step(i, carry):
        for u in range(SPREAD_UNROLL):
            chunk(pl.multiple_of((SPREAD_UNROLL * i + u) * n, n))
        return carry

    lax.fori_loop(0, ATOMS_DEV // (n * SPREAD_UNROLL), step, 0)


def wide_x_tables(cells, weights, slopes):
    columns = []
    for group in range(cells.shape[1] // 128):
        lanes = slice(128 * group, 128 * group + 128)
        columns.append(
            x_tables(
                cells[:, lanes],
                high_low([w[2:3, lanes] for w in weights])
                + high_low([w[2:3, lanes] for w in slopes]),
            )
        )
    return [jnp.concatenate(part, 1) for part in zip(*columns)]


def hold_x_tables(pieces, frac_ref, cell_ref, held):
    def step(index, carry):
        place = pl.ds(pl.multiple_of(index * 256, 256), 256)
        t = frac_ref[:, place]
        tables = wide_x_tables(cell_ref[:, place], spline_weights(t), spline_slopes(t))
        for k, table in enumerate(tables):
            held[k, index] = table
        return carry

    lax.fori_loop(*pieces, step, 0)


def gather_atoms(
    chunks, own, rim, charge_ref, frac_ref, cell_ref, out_ref, p_hi, p_lo, held=None, after_first=None
):
    base = 0 if own else CORE
    rows = slice(base, ROWS if rim else CORE)
    n = 256

    def piece_of(index):
        first = pl.multiple_of(index * n, n)
        t = frac_ref[:, pl.ds(first, n)]
        cells_all = cell_ref[:, pl.ds(first, n)]
        weights_all, slopes_all = spline_weights(t), spline_slopes(t)
        if held is None:
            w_hi, w_lo, s_hi, s_lo = wide_x_tables(cells_all, weights_all, slopes_all)
        else:
            w_hi, w_lo, s_hi, s_lo = (held[k, index] for k in range(4))
        hi, lo = p_hi[rows, :], p_lo[rows, :]
        along_all = nn_dot(hi, w_hi) + nn_dot(hi, w_lo) + nn_dot(lo, w_hi)
        steep_all = nn_dot(hi, s_hi) + nn_dot(hi, s_lo) + nn_dot(lo, s_hi)
        results = []
        for group in range(n // 128):
            lanes = slice(128 * group, 128 * group + 128)
            along, steep = along_all[:, lanes], steep_all[:, lanes]
            weights = [w[:, lanes] for w in weights_all]
            slopes = [w[:, lanes] for w in slopes_all]
            cells = cells_all[:, lanes]
            zw_main, zw_halo = narrow_tables(cells, weights, 0)
            zs_main, zs_halo = narrow_tables(cells, slopes, 0)
            yw_main, yw_halo = narrow_tables(cells, weights, 1)
            ys_main, ys_halo = narrow_tables(cells, slopes, 1)
            sums = [jnp.zeros((16, 128), F32)] * 3
            for y in range(0 if own else 16, 19 if rim else 16):
                row = 16 * y if y < 16 else 320 + 16 * (y - 16) - base
                yw = wide(yw_main[y : y + 1] if y < 16 else yw_halo[y - 16 : y - 15], 16)
                ys = wide(ys_main[y : y + 1] if y < 16 else ys_halo[y - 16 : y - 15], 16)
                piece, slope = along[row : row + 16], steep[row : row + 16]
                sums = [sums[0] + yw * piece, sums[1] + ys * piece, sums[2] + yw * slope]
            rims = [jnp.zeros((8, 128), F32)] * 3
            for pair in range(10 if rim else 0):
                row = (256 + 8 * pair if pair < 8 else 368 + 8 * (pair - 8)) - base
                yw = pair_pattern(yw_main, pair) if pair < 8 else pair_pattern(yw_halo, pair - 8)
                ys = pair_pattern(ys_main, pair) if pair < 8 else pair_pattern(ys_halo, pair - 8)
                piece, slope = along[row : row + 8], steep[row : row + 8]
                rims = [rims[0] + yw * piece, rims[1] + ys * piece, rims[2] + yw * slope]
            sums = [sums[0] * zs_main, sums[1] * zw_main, sums[2] * zw_main]
            rims = [rims[0] * zs_halo, rims[1] * zw_halo, rims[2] * zw_halo]
            results.append(
                jnp.concatenate(
                    [
                        jnp.sum(f[:8] + f[8:] + r, axis=0, keepdims=True)
                        for f, r in zip(sums, rims)
                    ],
                    0,
                )
            )
        q = charge_ref[:, pl.ds(first, n)]
        result = jnp.concatenate(results, 1) * -q
        if not own:
            result = result + out_ref[:, pl.ds(first, n)]
        out_ref[:, pl.ds(first, n)] = result

    low, high = chunks
    per_step = GATHER_UNROLL * CHUNK

    def step(i, carry):
        for u in range(per_step // n):
            piece_of(low * (CHUNK // n) + i * (per_step // n) + u)
        if after_first is not None:
            pl.when(i == 0)(after_first)
        return carry

    lax.fori_loop(0, (high - low) // GATHER_UNROLL, step, 0)


def turn(arrays):
    arrays = list(arrays)
    rows = arrays[0].shape[0]
    group = lax.broadcasted_iota(jnp.int32, (rows, 128), 1) >> 2
    for bit in range(4):
        g = 1 << bit
        keep = (group & g) == 0
        fresh = list(arrays)
        for i in range(16):
            if i & g == 0:
                low, high = arrays[i], arrays[i | g]
                fresh[i] = jnp.where(keep, low, pltpu.roll(high, 4 * g, 1))
                fresh[i | g] = jnp.where(keep, pltpu.roll(low, 128 - 4 * g, 1), high)
        arrays = fresh
    return arrays


def tables_of_influence(moduli_ref, screening, a, b, outs):
    m = [moduli_ref[c : c + 1, :] for c in range(3)]
    lane_k = lax.broadcasted_iota(jnp.int32, (256, 256), 1)
    row_k = lax.broadcasted_iota(jnp.int32, (256, 256), 0)
    same = lane_k == row_k
    other = lane_k == ((256 - row_k) & 255)

    def column(row, mask):
        return jnp.sum(jnp.where(mask, wide(row, 256), 0.0), axis=1, keepdims=True)

    m0, m1, m2 = column(m[0], same), column(m[1], same), column(m[2], same)
    m1_back = column(m[1], other)

    lane = lax.broadcasted_iota(jnp.int32, (1, 128), 1)
    local, j = (lane >> 2) & 15, lane & 3
    step = 8 * b + (local >> 1)
    kz = jnp.where(local & 1 == 0, step, jnp.where(step == 0, 128, 256 - step))
    rows = lax.broadcasted_iota(jnp.int32, (256, 128), 0)

    def along_lanes(col, index):
        hit = rows == wide(index, 256)
        return jnp.sum(jnp.where(hit, jnp.broadcast_to(col, (256, 128)), 0.0), 0, keepdims=True)

    z0, z1 = along_lanes(m0, kz), along_lanes(m0, (256 - kz) & 255)
    def signed(k):
        return jnp.where(k < 128, k, k - 256)

    nz, ny = signed(kz), signed(rows)
    flat = ny * ny + wide(nz * nz, 256)

    def kernel_at(kx):
        nx = signed(kx)
        radius = flat + wide(nx * nx, 256)
        squared = radius.astype(F32) / float(GRID * GRID)
        safe = jnp.where(radius > 0, squared, 1.0)
        first, second = along_lanes(m2, kx), along_lanes(m2, (256 - kx) & 255)
        product = m1 * wide(z0 * first, 256) + m1_back * wide(z1 * second, 256)
        value = product * jnp.exp(-screening * squared) / safe
        return jnp.where(radius > 0, value, 0.0) * (1.0 / float(GRID * GRID))

    kx = 8 * a + j
    at_first, at_last = kernel_at(kx), kernel_at(jnp.full_like(kx, 128))
    packed = wide(kx, 256) == 0
    outs[0][...] = jnp.where(packed, 0.5 * (at_first + at_last), at_first)
    outs[1][...] = kernel_at(kx + 4)
    outs[2][...] = jnp.where(packed, 0.5 * (at_first - at_last), 0.0)


def block(ref, index):
    return ref[:, BLOCK * index : BLOCK * index + BLOCK]


def shift_left(blocks, amount, top, keep):
    bit = top
    while bit:
        take = wide((amount & bit) > 0, blocks[0].shape[0])
        count = min(len(blocks), keep + bit - 1)
        last = len(blocks) - 1
        blocks = [
            jnp.where(take, blocks[min(i + bit, last)], blocks[i]) for i in range(count)
        ]
        bit //= 2
    return blocks


def handed_first(live, kept, charge_ref, frac_ref, cell_ref, charge_out, frac_out, cell_out):
    home = NBLK - SEND_MAX
    start = jnp.minimum(jnp.full((1, BLOCK), kept, jnp.int32), home)
    count = jnp.full((1, BLOCK), live, jnp.int32)
    charges = [jnp.where(count > i, block(charge_ref, i), 0.0) for i in range(NBLK)]
    for blocks, out in (
        (charges, charge_out),
        ([block(frac_ref, i) for i in range(NBLK)], frac_out),
        ([block(cell_ref, i) for i in range(NBLK)], cell_out),
    ):
        ordered = shift_left(blocks, start, 32, SEND_MAX) + blocks[:home]
        for i, value in enumerate(ordered):
            out[:, BLOCK * i : BLOCK * i + BLOCK] = value


def place_forces(kept, kept_before, arriving, forces, guests, out_ref):
    home = NBLK - SEND_MAX
    kept = jnp.full((1, BLOCK), kept, jnp.int32)
    kept_before = jnp.full((1, BLOCK), kept_before, jnp.int32)
    end = kept + arriving
    skip = kept_before - jnp.minimum(kept_before, home)
    arrived = shift_left([block(guests, i) for i in range(SEND_MAX)], skip, 32, SEND_MAX)
    placed = arrived + [jnp.zeros((3, BLOCK), F32)] * (NBLK - SEND_MAX)
    bit = 64
    while bit:
        take = wide((kept & bit) > 0, 3)
        placed = [
            jnp.where(take, placed[i - bit] if i >= bit else 0.0, placed[i]) for i in range(NBLK)
        ]
        bit //= 2
    for slot in range(NBLK):
        own = block(forces, SEND_MAX + slot if slot < home else slot - home)
        guest = jnp.where(wide(end > slot, 3), placed[slot], 0.0)
        out_ref[:, BLOCK * slot : BLOCK * slot + BLOCK] = jnp.where(wide(kept > slot, 3), own, guest)


def offsets_z():
    return [(dz, dy) for dz in (4, 3, -3, 2, -2, 1, -1, 0) for dy in (1, 0) if (dz, dy) != (0, 0)]


def offsets_y():
    moves = [(dx, dy, dc) for dx in (2, 1, -1, 0) for dy in (1, 0) for dc in (1, 0)]
    moves.remove((0, 0, 0))
    return sorted(moves, key=lambda m: -(abs(m[0]) + 2 * m[1]))


def solve_kernel(
    live_ref,
    send_ref,
    screening_ref,
    charge_ref,
    frac_ref,
    cell_ref,
    moduli_ref,
    fx_far,
    gx_far,
    fz_far,
    gz_far,
    fy_far,
    out_ref,
    fx,
    gx,
    fz,
    gz,
    fy,
    table_sems,
    tile_ref,
    pot_ref,
    rim_in,
    planes_out,
    send_1,
    recv_1,
    send_2,
    recv_2,
    send_3,
    recv_3,
    send_4,
    recv_4,
    straight_0,
    straight_1,
    crossed_0,
    p_hi,
    p_lo,
    forces,
    guests,
    charge_in_order,
    frac_in_order,
    cell_in_order,
    held,
    held_1,
    held_4,
    rim_sems,
    relay_sems,
    send_sems,
    recv_sems,
):
    a, b = lax.axis_index("gz"), lax.axis_index("gy")
    barrier = pltpu.get_barrier_semaphore()
    peers_z = [
        ((a // 2 + dz + 8) % 8) * 2 + (a + dy) % 2 for dz, dy in offsets_z()
    ]
    peers_y = [
        ((b // 4 + dx + 4) % 4) * 4 + ((b // 2 + dy) % 2) * 2 + (b + dc) % 2
        for dx, dy, dc in offsets_y()
    ]
    for peer in peers_z:
        pl.semaphore_signal(barrier, inc=1, device_id=(peer, b), device_id_type=MESH)
    for peer in peers_y:
        pl.semaphore_signal(barrier, inc=1, device_id=(a, peer), device_id_type=MESH)

    loads = [
        pltpu.make_async_copy(far, near, table_sems.at[k])
        for k, (far, near) in enumerate(
            ((fx_far, fx), (fz_far, fz), (fy_far, fy), (gz_far, gz), (gx_far, gx))
        )
    ]
    for load in loads:
        load.start()

    before, after = (b + 15) % 16, (b + 1) % 16
    before_z, after_z = (a + 15) % 16, (a + 1) % 16
    for peer in ((before_z, before), (after_z, after)):
        pl.semaphore_signal(barrier, inc=1, device_id=peer, device_id_type=MESH)
    live = live_ref[0, b]
    kept = live - send_ref[0, b]
    kept_before = live_ref[0, before] - send_ref[0, before]
    arriving = send_ref[0, before]
    spread_atoms(live * BLOCK, charge_ref, frac_ref, cell_ref, tile_ref)
    for load in loads:
        load.wait()
    pl.semaphore_wait(barrier, 2 * NPEER)

    leaving = []

    def exchange(stage, src, dst, size, over_z, relay=None):
        me = a if over_z else b
        peers = peers_z if over_z else peers_y
        whole = pl.ds(0, (NPEER - 1) * size)

        def rows_of(index):
            return pl.ds(pl.multiple_of(index * size, 8), size)

        def copy(source, target, peer, send_sem, recv_sem):
            return pltpu.make_async_remote_copy(
                src_ref=source,
                dst_ref=target,
                send_sem=send_sem,
                recv_sem=recv_sem,
                device_id=(peer, b) if over_z else (a, peer),
                device_id_type=MESH,
            )

        send_sem, recv_sem = send_sems.at[stage], recv_sems.at[stage]
        passing = []
        if relay is not None:
            buffer, sems = relay
            step = (a // 2 + 6) % 8 * 2
            origin = (a // 2 + 2) % 8 * 2 + a % 2
            for k in range(2):
                leg = buffer.at[pl.ds(k * size, size), :]
                copy(
                    src.at[rows_of(peers[k]), :], leg, step + a % 2, send_sem, relay_sems.at[sems]
                ).start()
                passing.append(
                    copy(
                        leg,
                        dst.at[rows_of(origin), :],
                        step + (a + 1 - k) % 2,
                        relay_sems.at[sems + 1],
                        recv_sem,
                    )
                )
            peers = peers[2:]
        for peer in peers:
            copy(src.at[rows_of(peer), :], dst.at[rows_of(me), :], peer, send_sem, recv_sem).start()
        dst[rows_of(me), :] = src[rows_of(me), :]
        every = copy(src.at[whole, :], dst.at[whole, :], peers[0], send_sem, recv_sem)
        leaving.append(every.wait_send)
        if relay is not None:
            both = pl.ds(0, 2 * size)
            legs = copy(
                buffer.at[both, :],
                buffer.at[both, :],
                peers[0],
                relay_sems.at[sems + 1],
                relay_sems.at[sems],
            )
            leaving.append(legs.wait_send)

            def forward():
                legs.wait_recv()
                for message in passing:
                    message.start()

            return every.wait_recv, forward
        return every.wait_recv

    def rim_copy(index, source, target, peer):
        return pltpu.make_async_remote_copy(
            src_ref=source,
            dst_ref=target,
            send_sem=rim_sems.at[2 * index],
            recv_sem=rim_sems.at[2 * index + 1],
            device_id=peer,
            device_id_type=MESH,
        )

    rims = [
        rim_copy(k, tile_ref.at[pl.ds(first, size), :], rim_in.at[pl.ds(first - 256, size), :], peer)
        for k, (first, size, peer) in enumerate(
            ((368, 16, (after_z, after)), (256, 64, (after_z, b)), (320, 48, (a, after)))
        )
    ]
    for copy in rims:
        copy.start()

    def transform_x(value):
        high, low = split(value)
        return nn_dot(high, fx[0]) + nn_dot(high, fx[1]) + nn_dot(low, fx[0])

    spectrum = transform_x(tile_ref[0:256, :])
    handed_first(
        live, kept, charge_ref, frac_ref, cell_ref, charge_in_order, frac_in_order, cell_in_order
    )
    hold_x_tables((0, 16), frac_in_order, cell_in_order, held)
    for copy in rims:
        copy.wait()
    extra = transform_x(rim_in[...])
    iota = lax.broadcasted_iota(jnp.int32, (8, 256), 0)
    planes = [spectrum[16 * y : 16 * y + 16] for y in range(16)]
    for y in range(16):
        halo = extra[8 * (y // 2) : 8 * (y // 2) + 8]
        if y < 4:
            halo = halo + extra[112 + 8 * (y // 2) : 120 + 8 * (y // 2)]
        halo = jnp.where(iota < 4, halo if y % 2 == 0 else pltpu.roll(halo, 4, 0), 0.0)
        plane = jnp.concatenate([planes[y][:8] + halo, planes[y][8:]], 0)
        planes[y] = plane + extra[64 + 16 * y : 80 + 16 * y] if y < 3 else plane

    def send_lines(stream):
        lanes = slice(128 * stream, 128 * stream + 128)
        for peer, piece in enumerate(turn([plane[:, lanes] for plane in planes])):
            first = 256 * stream + 16 * peer
            send_1[first : first + 16, :] = piece

    def part(ref, stream):
        return ref.at[pl.ds(256 * stream, 256), :]

    send_lines(0)
    arrive_10 = exchange(0, part(send_1, 0), part(recv_1, 0), 16, True)
    send_lines(1)
    arrive_11, forward = exchange(1, part(send_1, 1), part(recv_1, 1), 16, True, (held_1, 0))
    tables_of_influence(
        moduli_ref, screening_ref[0], a, b, (straight_0, straight_1, crossed_0)
    )
    hold_x_tables((16, EARLY * CHUNK // 256), frac_in_order, cell_in_order, held)
    forward()

    half = lax.broadcasted_iota(jnp.int32, (1, 128), 1) < 64
    forward_sign = jnp.where(half, 1.0, -1.0)

    def product(table, value):
        high, low = split(value)
        width = value.shape[1]
        both = nn_dot(table[0], jnp.concatenate([high, low], 1))
        return both[:, :width] + both[:, width:] + nn_dot(table[1], high)

    def joined(both, sign):
        rows = both.shape[0] // 2
        return both[:rows] + wide(sign, rows) * pltpu.roll(both[rows:], 64, 1)

    def stage_z(stream):
        lines = recv_1[256 * stream : 256 * stream + 256, :]
        waves = joined(product(fz, lines), forward_sign)
        turned = turn([waves[16 * k : 16 * k + 16] for k in range(16)])
        for y in range(16):
            send_2[pl.ds(256 * stream + y, 16, stride=16), :] = turned[y]
        return exchange(2 + stream, part(send_2, stream), part(recv_2, stream), 16, False)

    def stage_y(stream):
        lines = recv_2[256 * stream : 256 * stream + 256, :]
        if stream == 0:
            lane = lax.broadcasted_iota(jnp.int32, (256, 128), 1)
            odd = (lane >> 2) & 1
            swapped = jnp.where(odd == 0, pltpu.roll(lines, 124, 1), pltpu.roll(lines, 4, 1))
            own_pair = wide(((lax.broadcasted_iota(jnp.int32, (1, 128), 1) & 63) >> 3) + b, 256) == 0
            swapped = jnp.where(own_pair, lines, swapped)
            both = product(fy, jnp.concatenate([lines, swapped * wide(forward_sign, 256)], 1))
            waves = joined(both[:, :128], forward_sign) * straight_0[...]
            waves = waves + joined(both[:, 128:], forward_sign) * crossed_0[...]
        else:
            waves = joined(product(fy, lines), forward_sign) * straight_1[...]
        first = 256 * stream
        send_3[first : first + 256, :] = joined(product(fy, waves), -forward_sign)
        return exchange(4 + stream, part(send_3, stream), part(recv_3, stream), 16, False)

    def stage_z_back(stream):
        pieces = [recv_3[pl.ds(256 * stream + y, 16, stride=16), :] for y in range(16)]
        lines = jnp.concatenate(turn(pieces), 0)
        first = 256 * stream
        send_4[first : first + 256, :] = joined(product(gz, lines), -forward_sign)
        relay = (held_4, 2) if stream else None
        return exchange(6 + stream, part(send_4, stream), part(recv_4, stream), 16, True, relay)

    arrive_10()
    arrive_20 = stage_z(0)
    arrive_11()
    arrive_21 = stage_z(1)
    arrive_20()
    arrive_30 = stage_y(0)
    arrive_21()
    arrive_31 = stage_y(1)
    arrive_30()
    arrive_40 = stage_z_back(0)
    arrive_31()
    arrive_41, forward = stage_z_back(1)
    forward()
    def lines_back(stream):
        return turn(
            [recv_4[256 * stream + 16 * k : 256 * stream + 16 * k + 16, :] for k in range(16)]
        )

    arrive_40()
    turned_0 = lines_back(0)
    arrive_41()
    turned_1 = lines_back(1)

    high, low = split(
        jnp.concatenate([jnp.concatenate(pair, 1) for pair in zip(turned_0, turned_1)], 0)
    )
    value = nn_dot(high, gx[0]) + nn_dot(high, gx[1]) + nn_dot(low, gx[0])
    pot_ref[0:256, :] = value
    for pair in range(8):
        even, odd = value[32 * pair : 32 * pair + 8], value[32 * pair + 16 : 32 * pair + 24]
        planes_out[8 * pair : 8 * pair + 8, :] = jnp.where(iota < 4, even, pltpu.roll(odd, 4, 0))
    copies = [
        rim_copy(3 + k, source.at[pl.ds(0, size), :], pot_ref.at[pl.ds(target, size), :], peer)
        for k, (source, target, size, peer) in enumerate(
            (
                (planes_out, 368, 16, (before_z, before)),
                (planes_out, 256, 64, (before_z, b)),
                (pot_ref, 320, 48, (a, before)),
            )
        )
    ]
    for copy in copies:
        copy.start()
    for leave in leaving:
        leave()

    def keep_parts(rows):
        high, low = split(pot_ref[rows, :])
        p_hi[rows, :] = high
        p_lo[rows, :] = low

    def compute(*split_of, **options):
        atoms = (charge_in_order, frac_in_order, cell_in_order)
        gather_atoms(*split_of, *atoms, forces, p_hi, p_lo, **options)

    hand_on = rim_copy(6, forces.at[:, pl.ds(0, SEND_MAX * BLOCK)], guests, (a, after))
    keep_parts(slice(0, CORE))
    compute((0, EARLY), True, False, held=held)
    for copy in copies:
        copy.wait()
    keep_parts(slice(CORE, ROWS))
    compute((0, EARLY), False, True, held=held)
    compute((EARLY, ATOMS_DEV // CHUNK), True, True, after_first=hand_on.start)
    hand_on.wait()
    place_forces(kept, kept_before, arriving, forces, guests, out_ref)


def solve(live_blocks, send_blocks, screening, charge, fractions, cells, moduli):
    tables = []
    for table in (forward_x(), inverse_x(), *tables_z(), table_y()):
        tables.append(jnp.asarray(np.stack(split_np(table))))
    short, both = pltpu.VMEM((256, 128), F32), pltpu.VMEM((512, 128), F32)
    return pl.pallas_call(
        solve_kernel,
        out_shape=jax.ShapeDtypeStruct((3, ATOMS_DEV), F32),
        in_specs=[pl.BlockSpec(memory_space=pltpu.SMEM)] * 3
        + [pl.BlockSpec(memory_space=pltpu.VMEM)] * 4
        + [pl.BlockSpec(memory_space=pltpu.HBM)] * len(tables),
        out_specs=pl.BlockSpec(memory_space=pltpu.VMEM),
        scratch_shapes=[pltpu.VMEM(table.shape, BF16) for table in tables]
        + [pltpu.SemaphoreType.DMA((len(tables),))]
        + [pltpu.VMEM((ROWS, GRID), F32)] * 2
        + [pltpu.VMEM((128, GRID), F32), pltpu.VMEM((64, GRID), F32)]
        + [both] * 8
        + [short] * 3
        + [pltpu.VMEM((ROWS, GRID), BF16)] * 2
        + [
            pltpu.VMEM((3, ATOMS_DEV), F32),
            pltpu.VMEM((3, SEND_MAX * BLOCK), F32),
            pltpu.VMEM((1, ATOMS_DEV), F32),
            pltpu.VMEM((3, ATOMS_DEV), F32),
            pltpu.VMEM((3, ATOMS_DEV), jnp.int32),
            pltpu.VMEM((4, EARLY * CHUNK // 256, 256, 256), BF16),
            pltpu.VMEM((32, 128), F32),
            pltpu.VMEM((32, 128), F32),
            pltpu.SemaphoreType.DMA((14,)),
            pltpu.SemaphoreType.DMA((4,)),
            pltpu.SemaphoreType.DMA((8,)),
            pltpu.SemaphoreType.DMA((8,)),
        ],
        compiler_params=pltpu.CompilerParams(collective_id=0, has_side_effects=True),
        name="forces",
    )(live_blocks, send_blocks, screening, charge, fractions, cells, moduli, *tables)


def body(charge, fractions, cell_base, live_blocks, send_blocks, moduli, screening):
    return solve(
        live_blocks, send_blocks, screening, charge[None, :], fractions, cell_base, moduli
    )


def solution(mesh):
    return jax.shard_map(
        body,
        mesh=mesh,
        in_specs=(
            P(("gz", "gy")),
            P(None, ("gz", "gy")),
            P(None, ("gz", "gy")),
            P("gz", None),
            P("gz", None),
            P(),
            P(),
        ),
        out_specs=P(None, ("gz", "gy")),
        check_vma=False,
    )
```
